32 devices in a mesh: dp: 2 (over y), shard: 16 (over z, x, core).
Axes of the slice: x: 2, y: 2, z: 4, core: 2. Of those that a mesh axis runs over, the one named last changes fastest.
Arguments:
- gradients: bfloat16 [2, 16, 2, 786432], P('dp', 'shard'), may hold values from -6 to 6
- tile_table: int32 [16, 96], replicated, may hold values from 0 to 1535, as said below
- master: float32 [16, 2, 786432], P('shard', 'dp'), may hold values from -0.072 to 0.072
- moment: float32 [16, 2, 786432], P('shard', 'dp'), may hold values from -6 to 6
- second: float32 [16, 2, 786432], P('shard', 'dp'), may hold values from 1 to 16
Outputs:
- master_new: float32 [16, 2, 786432], P('shard', 'dp')
- moment_new: float32 [16, 2, 786432], P('shard', 'dp')
- second_new: float32 [16, 2, 786432], P('shard', 'dp')
- tiles_out: bfloat16 [1536, 128, 128], P('shard')
- scales_out: bfloat16 [1536], P('shard')
The draws below stay inside these ranges and needn't reach their ends.
Inputs may be any that keep to these rules, and one draw needn't show every extreme that they name: tile_table holds each number of 0 to 1535 once; each row holds exactly 6 numbers of every block of 96 consecutive numbers; in any row, the columns d * 48 to (d + 1) * 48 - 1 hold at most 3 numbers of one block, and this most is reached; over all rows together those columns hold exactly 48 numbers of every block.
All inputs are finite; a program needn't handle non-finite values.
Results may differ from the reference program's by a relative error of at most 0.0095.
Values may be sent and summed in bfloat16 or wider, within the bound.
No kernel may reach another device: no remote copies, remote signals or barrier semaphores. Data moves between devices by JAX's collectives and lax.ppermute only.
A program may use at most 64 MiB of HBM per device.

```python
import math
import jax
import jax.numpy as jnp
from jax import lax

TB = 128
TILES_OWNER = 96
SHARD_LEN = 786432
N_DP = 2
N_SHARD = 16


def shuffle_row(key, row_values):
    return jax.random.permutation(key, row_values)


def owner_permutation(key):
    return jax.random.permutation(key, TILES_OWNER)


def draw_tile_table(key, part):
    sub_len = TILES_OWNER // N_DP
    per_pair = TILES_OWNER // N_SHARD
    shifts = jax.random.permutation(jax.random.fold_in(key, 31), N_SHARD).astype(jnp.int32)
    relabel = jax.random.permutation(jax.random.fold_in(key, 32), N_SHARD).astype(jnp.int32)
    position = jnp.arange(TILES_OWNER, dtype=jnp.int32)
    cyclic = (position[None, :] + shifts[:, None]) % N_SHARD
    labels = relabel[cyclic].reshape(N_SHARD * N_DP, sub_len)
    block_keys = jax.random.split(jax.random.fold_in(key, 33), N_SHARD * N_DP)
    labels = jax.vmap(shuffle_row)(block_keys, labels).reshape(N_SHARD, TILES_OWNER).astype(jnp.int32)
    same = labels[:, :, None] == labels[:, None, :]
    earlier = position[None, :] < position[:, None]
    row_rank = jnp.sum(jnp.logical_and(same, earlier[None]), axis=-1).astype(jnp.int32)
    occurrence = jnp.arange(N_SHARD, dtype=jnp.int32)[:, None] * per_pair + row_rank
    owner_keys = jax.random.split(jax.random.fold_in(key, 34), N_SHARD)
    perms = jax.vmap(owner_permutation)(owner_keys).astype(jnp.int32)
    slots = labels * TILES_OWNER + perms[labels, occurrence]
    return slots.astype(jnp.int32)


def draw_master(key, part):
    shape = (N_SHARD, N_DP, SHARD_LEN // TB, TB)
    base = jnp.clip(jax.random.normal(jax.random.fold_in(key, 21), shape, jnp.float32), -6.0, 6.0)
    row_scale = jnp.exp(jax.random.uniform(jax.random.fold_in(key, 22), shape[:3] + (1,), jnp.float32, 0.0, math.log(10.0)))
    factor = 0.0012
    values = factor * base * row_scale
    return values.reshape(N_SHARD, N_DP, SHARD_LEN).astype(jnp.float32)


def spiked(values, rng, source, target, shards_of, factor):
    owner, partner = [(jnp.arange(values.shape[dim]) // (values.shape[dim] // shards_of)).reshape([-1 if axis == dim else 1 for axis in range(values.ndim)]) for dim in (source, target)]
    chosen = jax.random.permutation(rng, shards_of)[partner]
    strong = (owner == chosen) | (owner == (partner + shards_of // 2) % shards_of)
    return jnp.where(strong, factor * values, values)


def block_levels(own_key, dims, shards, low, high):
    level = 1.0
    for dim, shards_of in shards:
        heights = jax.random.uniform(jax.random.fold_in(jax.random.fold_in(own_key, 6), dim), (shards_of,), jnp.float32, low / len(shards), high / len(shards))
        level = level * jnp.repeat(jnp.exp(heights), dims[dim] // shards_of).reshape((-1,) + (1,) * (len(dims) - 1 - dim))
    return level


def noise(rng, shape, spread, most, pieces=(), kind=jnp.bfloat16):
    drawn = spread * jax.random.normal(rng, shape, jnp.float32)
    if pieces:
        drawn = drawn * block_levels(rng, shape, pieces, -0.22, 0.18)
    return jnp.clip(drawn, -most, most).astype(kind)


def heavy_noise(own_key, shape, deviation, reach, shards, heavy, kind=jnp.bfloat16):
    result = deviation * jax.random.normal(own_key, shape, jnp.float32)
    if shards:
        result = result * block_levels(own_key, shape, shards, -0.22, 0.18)
    return jnp.clip(spiked(result, jax.random.fold_in(own_key, 3), *heavy), -reach, reach).astype(kind)


def setup_inputs(seed: int = 0) -> dict:
    key_list = jax.random.split(jax.random.key(seed), 6)
    return {
        "gradients": heavy_noise(key_list[0], (N_DP, N_SHARD, N_DP, SHARD_LEN), 1.0, 6.0, ((0, 2), (1, 16)), (0, 2, 2, 2.0)),
        "tile_table": draw_tile_table(jax.random.fold_in(key_list[5], 71), 0),
        "master": draw_master(jax.random.fold_in(key_list[5], 71), 0),
        "moment": noise(key_list[3], (N_SHARD, N_DP, SHARD_LEN), 1.0, 6.0, ((0, 16), (1, 2)), jnp.float32),
        "second": jnp.clip(jnp.exp(math.log(16.0) - 2.7725887 * jax.random.uniform(key_list[4], (N_SHARD, N_DP, SHARD_LEN), jnp.float32) ** block_levels(key_list[4], (N_SHARD, N_DP, SHARD_LEN), ((0, 16), (1, 2)), -0.2, 0.2)), 1.0, 16.0),
    }


beta_first = 0.9
beta_second = 0.95
learning_rate = 0.002
weight_decay = 0.1
adam_epsilon = 1e-08
scale_epsilon = 1e-06
step_count = 10

def reference(gradients, tile_table, master, moment, second):
    grad = lax.optimization_barrier(jnp.sum(gradients.astype(jnp.float32), axis=0))
    moment_new = beta_first * moment + (1.0 - beta_first) * grad
    second_new = beta_second * second + (1.0 - beta_second) * grad * grad
    first_fix = 1.0 - beta_first ** step_count
    second_fix = 1.0 - beta_second ** step_count
    update = moment_new / first_fix / (jnp.sqrt(second_new / second_fix) + adam_epsilon)
    master_new = master - learning_rate * (update + weight_decay * master)
    tile_set = master_new.reshape(-1, TB, TB)
    largest = lax.optimization_barrier(jnp.max(jnp.abs(tile_set), axis=(1, 2)))
    tile_scale = (largest + scale_epsilon).astype(jnp.bfloat16)
    quantized = (tile_set / tile_scale.astype(jnp.float32)[:, None, None]).astype(jnp.bfloat16)
    slots = tile_table.reshape(-1).astype(jnp.int32)
    tiles_out = jnp.zeros_like(quantized).at[slots].set(quantized)
    scales_out = jnp.zeros(tile_scale.shape, jnp.bfloat16).at[slots].set(tile_scale)
    return (master_new, moment_new, second_new, tiles_out, scales_out)
```

```python
import functools

import jax
import jax.numpy as jnp
from jax import lax
from jax.experimental import pallas as pl
from jax.experimental.pallas import tpu as pltpu
from jax.sharding import PartitionSpec as P


TB = 128
LANES = 128

beta_first = 0.9
beta_second = 0.95
learning_rate = 0.002
weight_decay = 0.1
adam_epsilon = 1e-08
scale_epsilon = 1e-06
step_count = 10

HBM = pl.BlockSpec(memory_space=pltpu.HBM)
VMEM = pl.BlockSpec(memory_space=pltpu.VMEM)
SMEM = pl.BlockSpec(memory_space=pltpu.SMEM)


def in_hbm(arrays):
    return [pltpu.with_memory_space_constraint(a, pltpu.HBM) for a in arrays]


def rank_within(owners):
    position = jnp.arange(owners.shape[-1], dtype=jnp.int32)
    same_owner = owners[..., :, None] == owners[..., None, :]
    earlier = position[None, :] < position[:, None]
    return jnp.sum((same_owner & earlier).astype(jnp.int32), axis=-1)


def extract(raw, wide, part, parts):
    wide[...] = raw[...].astype(jnp.float32)
    return wide[pl.ds(part, TB, stride=parts), :]


def fill_order(part, table, row, owners, parts, room, owned, order, count):
    sub_len = owned // parts

    def clear(k, carry):
        order[part * room * owners + k] = 0
        return carry

    def zero(k, carry):
        count[k] = 0
        return carry

    def enter(t, carry):
        owner = table[row, part * sub_len + t] // owned
        rank = count[owner]
        count[owner] = rank + 1
        order[(part * room + rank) * owners + owner] = t
        return carry

    if room * owners != sub_len:
        lax.fori_loop(0, room * owners, clear, 0)
    lax.fori_loop(0, owners, zero, 0, unroll=True)
    lax.fori_loop(0, sub_len, enter, 0, unroll=4)


def pack_kernel(chunk, shift, owners, parts, room, owned, lead, *refs):
    if lead:
        table, grads, order, out, raw, wide, sems, count = refs
        row = lax.axis_index("shard")
        fill = functools.partial(
            fill_order,
            table=table,
            row=row,
            owners=owners,
            parts=parts,
            room=room,
            owned=owned,
            order=order,
            count=count,
        )
        fill(lax.rem(lax.axis_index("dp") + shift, parts))
    else:
        order, grads, out, raw, wide, sems = refs
    part = lax.rem(lax.axis_index("dp") + shift, parts)
    base = (part * room + chunk) * owners
    slots = raw.shape[0]

    def fetch(i):
        slot = lax.rem(i, slots)
        return pltpu.make_async_copy(grads.at[order[base + i]], raw.at[slot], sems.at[slot])

    for i in range(min(slots, owners)):
        fetch(i).start()
    if lead:
        for s in range(parts - 1):
            fill(lax.rem(lax.axis_index("dp") + shift + 1 + s, parts))

    def body(i, carry):
        fetch(i).wait()
        out[i] = extract(raw.at[lax.rem(i, slots)], wide, part, parts).astype(out.dtype)

        @pl.when(i + slots < owners)
        def _():
            fetch(i + slots).start()

        return carry

    lax.fori_loop(0, owners, body, 0)


def adam_kernel(chunk, last, owners, parts, room, *refs):
    order, _, grads, master, moment, second = refs[:6]
    refs = refs[6:]
    if chunk:
        sc_in, refs = refs[0], refs[1:]
    arrived = refs[: parts - 1]
    refs = refs[parts - 1 + (3 if chunk else 0) :]
    outs = refs[:3]
    record = refs[3]
    sc_out = refs[4]
    raw, wide, states, news, peak, scale, quant, in_sems, out_sems, quant_sems = refs[5:]
    part = lax.axis_index("dp")
    base = (part * room + chunk) * owners

    def fetches(i):
        tile = order[base + i]
        copies = [pltpu.make_async_copy(grads.at[tile], raw.at[i], in_sems.at[0, i])]
        for k, ref in enumerate((master, moment, second)):
            copies.append(pltpu.make_async_copy(ref.at[tile], states.at[k, i], in_sems.at[k + 1, i]))
        return copies

    def stores(i):
        tile = order[base + i]
        return [pltpu.make_async_copy(news.at[k, i], outs[k].at[tile], out_sems.at[k, i]) for k in range(3)]

    def start_fetch(i, carry):
        for copy in fetches(i):
            copy.start()
        return carry

    lax.fori_loop(0, owners, start_fetch, 0)
    first_fix = 1.0 / (1.0 - beta_first**step_count)
    second_fix = 1.0 / (1.0 - beta_second**step_count)
    rows = 32

    def update(i, carry):
        for copy in fetches(i):
            copy.wait()
        wide[...] = raw[i].astype(jnp.float32)
        top = None
        for b in range(0, TB, rows):
            at = pl.ds(b, rows)
            grad = wide[pl.ds(b * parts + part, rows, stride=parts), :]
            for ref in arrived:
                grad = grad + ref[i, at, :].astype(jnp.float32)
            moment_new = beta_first * states[1, i, at, :] + (1.0 - beta_first) * grad
            second_new = beta_second * states[2, i, at, :] + (1.0 - beta_second) * grad * grad
            old = states[0, i, at, :]
            step = moment_new * first_fix / (jnp.sqrt(second_new * second_fix) + adam_epsilon)
            master_new = old - learning_rate * (step + weight_decay * old)
            news[0, i, at, :] = master_new
            news[1, i, at, :] = moment_new
            news[2, i, at, :] = second_new
            size = jnp.abs(master_new)
            for s in range(0, rows, 8):
                top = size[s : s + 8] if top is None else jnp.maximum(top, size[s : s + 8])
        peak[i] = top
        for copy in stores(i):
            copy.start()
        return carry

    lax.fori_loop(0, owners, update, 0)
    largest = jnp.max(jnp.max(peak[...], axis=2, keepdims=True), axis=1, keepdims=True)
    rounded = (largest + scale_epsilon).astype(jnp.bfloat16).astype(jnp.float32)
    rounded = jnp.broadcast_to(rounded, peak.shape)
    peak[...] = 1.0 / rounded
    row = lax.broadcasted_iota(jnp.int32, scale.shape, 1)
    scale[...] = jnp.where(row == chunk, jnp.broadcast_to(rounded[:, :1], scale.shape), sc_in[...] if chunk else 0.0)

    def send(i):
        return pltpu.make_async_copy(quant.at[i], record.at[i], quant_sems.at[i])

    def quantize(i, carry):
        inverse = peak[i]
        for b in range(0, TB, 16):
            pair = [news[0, i, pl.ds(b + s, 8), :] * inverse for s in (0, 8)]
            quant[i, pl.ds(b, 16), :] = jnp.concatenate(pair, axis=0).astype(quant.dtype)
        if last:
            quant[i, pl.ds(TB, scale.shape[1]), :] = scale[i].astype(quant.dtype)
        send(i).start()
        return carry

    lax.fori_loop(0, owners, quantize, 0)
    sc_out[...] = scale[...]

    def finish(i, carry):
        send(i).wait()
        for copy in stores(i):
            copy.wait()
        return carry

    lax.fori_loop(0, owners, finish, 0)


def place_kernel(sources, scale_sources, owners, room, owned, first, *refs):
    slots = refs[0]
    count = len(sources)
    records = refs[1 : 1 + count]
    scales = refs[1 + count : 1 + count + len(scale_sources)]
    refs = refs[1 + count + len(scale_sources) + (0 if first else 1) :]
    tiles_out = refs[0]
    if scale_sources:
        scales_out = refs[1]
    sems = refs[-1]
    here = lax.axis_index("dp")
    parts = slots.shape[0] // (room * owners)

    def index(chunk, shift, i):
        part = lax.rem(here + parts - shift, parts)
        return slots[(part * room + chunk) * owners + i]

    def copy(n, i, slot):
        return pltpu.make_async_copy(records[n].at[i, pl.ds(0, TB)], tiles_out.at[slot], sems.at[n, i])

    for n, (chunk, shift) in enumerate(sources):

        def start(i, carry, n=n, chunk=chunk, shift=shift):
            slot = index(chunk, shift, i)

            @pl.when(slot >= 0)
            def _():
                copy(n, i, slot).start()

            return carry

        lax.fori_loop(0, owners, start, 0)
    if scale_sources:
        lane = lax.broadcasted_iota(jnp.int32, scales_out.shape, 1)
        scales_out[...] = jnp.zeros(scales_out.shape, scales_out.dtype)
        for n, shift in enumerate(scale_sources):

            def gather(i, carry, n=n, shift=shift):
                block = scales[n][i, pl.ds(TB, scales[n].shape[1] - TB), :].astype(jnp.float32)
                total = scales_out[...]
                for r in range(room):
                    wide = jnp.concatenate([block[r : r + 1]] * (scales_out.shape[1] // LANES), axis=1)
                    total = jnp.where(lane == index(r, shift, i), wide, total)
                scales_out[...] = total
                return carry

            lax.fori_loop(0, owners, gather, 0)
    for n, (chunk, shift) in enumerate(sources):

        def end(i, carry, n=n, chunk=chunk, shift=shift):
            slot = index(chunk, shift, i)

            @pl.when(slot >= 0)
            def _():
                copy(n, i, slot).wait()

            return carry

        lax.fori_loop(0, owners, end, 0)


def per_device(gradients, tile_table, master, moment, second):
    owners = lax.axis_size("shard")
    parts = lax.axis_size("dp")
    owned = tile_table.shape[1]
    sub_len = owned // parts
    room = (sub_len + owners - 1) // owners
    me = lax.axis_index("shard")
    tiles = master.size // (TB * TB)
    pad = (room + 7) // 8 * 8

    cube = tile_table.reshape(owners, parts, sub_len)
    cube_owner = cube // owned
    cube_rank = rank_within(cube_owner)
    chunk_ids = jnp.arange(room, dtype=jnp.int32)
    mine = (cube_owner == me)[:, :, None, :] & (cube_rank[:, :, None, :] == chunk_ids[:, None])
    slots = jnp.sum(jnp.where(mine, cube[:, :, None, :] - me * owned + 1, 0), axis=-1) - 1
    slots = slots.transpose(1, 2, 0).reshape(-1)

    grads = gradients.reshape(parts, tiles, TB, TB).transpose(1, 2, 0, 3).reshape(tiles, TB * parts, TB)
    states = [a.reshape(tiles, TB, TB) for a in (master, moment, second)]
    tile_bytes = TB * TB * 2 * parts
    ring = max(2, min(owners, (4 << 20) // tile_bytes))
    perms = {s: [(d, (d + s) % parts) for d in range(parts)] for s in range(1, parts)}
    f32_tiles = pltpu.HBM((tiles, TB, TB), jnp.float32)

    arrived = []
    for r in range(room):
        got = []
        for s in range(1, parts):
            lead = r == 0 and s == 1
            result = pl.pallas_call(
                functools.partial(pack_kernel, r, s, owners, parts, room, owned, lead),
                out_shape=[jax.ShapeDtypeStruct((parts * room * owners,), jnp.int32)] * lead
                + [jax.ShapeDtypeStruct((owners, TB, TB), jnp.bfloat16)],
                in_specs=[SMEM, HBM],
                out_specs=[SMEM] * lead + [VMEM],
                scratch_shapes=[
                    pltpu.VMEM((ring, TB * parts, TB), jnp.bfloat16),
                    pltpu.VMEM((TB * parts, TB), jnp.float32),
                    pltpu.SemaphoreType.DMA((ring,)),
                ]
                + [pltpu.SMEM((owners,), jnp.int32)] * lead,
                compiler_params=pltpu.CompilerParams(vmem_limit_bytes=16 << 20),
                cost_estimate=pl.CostEstimate(flops=6000000, bytes_accessed=2 << 20, transcendentals=0),
            )(tile_table if lead else order, *in_hbm([grads]))
            if lead:
                order, packed = result
            else:
                (packed,) = result
            got.append(lax.ppermute(packed, "dp", perms[s]))
        arrived.append(got)

    news = []
    sc = []
    mine_r, theirs_r = [], []
    for r in range(room):
        last = r == room - 1
        height = TB + (pad if last else 0)
        count = 6 + len(sc) + parts - 1
        *news, record, scale_rows = pl.pallas_call(
            functools.partial(adam_kernel, r, last, owners, parts, room),
            out_shape=[f32_tiles] * 3
            + [pltpu.HBM((owners, height, TB), jnp.bfloat16), jax.ShapeDtypeStruct((owners, pad, LANES), jnp.float32)],
            in_specs=[SMEM, SMEM, HBM, HBM, HBM, HBM] + [VMEM] * (len(sc) + parts - 1) + [HBM] * len(news),
            out_specs=[HBM] * 4 + [VMEM],
            input_output_aliases={count + k: k for k in range(len(news))},
            scratch_shapes=[
                pltpu.VMEM((owners, TB * parts, TB), jnp.bfloat16),
                pltpu.VMEM((TB * parts, TB), jnp.float32),
                pltpu.VMEM((3, owners, TB, TB), jnp.float32),
                pltpu.VMEM((3, owners, TB, TB), jnp.float32),
                pltpu.VMEM((owners, 8, LANES), jnp.float32),
                pltpu.VMEM((owners, pad, LANES), jnp.float32),
                pltpu.VMEM((owners, height, TB), jnp.bfloat16),
                pltpu.SemaphoreType.DMA((4, owners)),
                pltpu.SemaphoreType.DMA((3, owners)),
                pltpu.SemaphoreType.DMA((owners,)),
            ],
            compiler_params=pltpu.CompilerParams(vmem_limit_bytes=40 << 20),
            cost_estimate=pl.CostEstimate(flops=30000000, bytes_accessed=8 << 20, transcendentals=0),
        )(order, slots, *in_hbm([grads, *states]), *sc, *arrived[r], *in_hbm(news))
        kept = lax.all_to_all(record, "shard", split_axis=0, concat_axis=0, tiled=True)
        sc = [scale_rows]
        mine_r.append(kept)
        theirs_r.append([])
        for s in range(1, parts):
            theirs_r[r].append(lax.ppermute(kept, "dp", perms[s]))

    early = [((r, 0), mine_r[r]) for r in range(room)]
    early += [((r, s), theirs_r[r][s - 1]) for r in range(room - 1) for s in range(1, parts)]
    late = [((room - 1, s), theirs_r[room - 1][s - 1]) for s in range(1, parts)]
    tiles_shape = pltpu.HBM((owned, TB, TB), jnp.bfloat16)
    width = (owned + LANES - 1) // LANES * LANES

    def place(group, scale_group, previous):
        outs = [tiles_shape]
        out_specs = [HBM]
        if scale_group:
            outs.append(jax.ShapeDtypeStruct((1, width), jnp.float32))
            out_specs.append(VMEM)
        count = 1 + len(group) + len(scale_group)
        return pl.pallas_call(
            functools.partial(
                place_kernel,
                [k for k, _ in group],
                [k for k, _ in scale_group],
                owners,
                room,
                owned,
                not previous,
            ),
            out_shape=outs,
            in_specs=[SMEM] + [VMEM] * (count - 1) + [HBM] * len(previous),
            out_specs=out_specs,
            input_output_aliases={count: 0} if previous else {},
            scratch_shapes=[pltpu.SemaphoreType.DMA((len(group), owners))],
            compiler_params=pltpu.CompilerParams(vmem_limit_bytes=16 << 20),
            name="place_late" if previous else "place_early",
        )(slots, *[a for _, a in group], *[a for _, a in scale_group], *in_hbm(previous))

    (tiles_out,) = place(early, [], [])
    scale_group = [(0, mine_r[-1])] + [(s, theirs_r[-1][s - 1]) for s in range(1, parts)]
    tiles_out, scales = place(late, scale_group, [tiles_out])
    scales_out = scales[0, :owned].astype(jnp.bfloat16)
    return (*[a.reshape(master.shape) for a in news], tiles_out, scales_out)


def solution(mesh):
    in_specs = (
        P("dp", "shard", None, None),
        P(),
        P("shard", "dp", None),
        P("shard", "dp", None),
        P("shard", "dp", None),
    )
    out_specs = (
        P("shard", "dp", None),
        P("shard", "dp", None),
        P("shard", "dp", None),
        P("shard", None, None),
        P("shard"),
    )

    return jax.shard_map(per_device, mesh=mesh, in_specs=in_specs, out_specs=out_specs, check_vma=False)
```

```python
import functools

import jax
import jax.numpy as jnp
from jax import lax
from jax.experimental import pallas as pl
from jax.experimental.pallas import tpu as pltpu
from jax.sharding import PartitionSpec as P


TB = 128
LANES = 128
UNROLL = 2
PACK_MIB = 4
ADAM_MIB = 4


beta_first = 0.9
beta_second = 0.95
learning_rate = 0.002
weight_decay = 0.1
adam_epsilon = 1e-08
scale_epsilon = 1e-06
step_count = 10

HBM = pl.BlockSpec(memory_space=pltpu.HBM)
VMEM = pl.BlockSpec(memory_space=pltpu.VMEM)
SMEM = pl.BlockSpec(memory_space=pltpu.SMEM)


def in_hbm(arrays):
    return [pltpu.with_memory_space_constraint(a, pltpu.HBM) for a in arrays]


def in_vmem(arrays):
    return [pltpu.with_memory_space_constraint(a, pltpu.VMEM) for a in arrays]


def extract(raw, wide, part, parts):
    wide[...] = raw[...].astype(jnp.float32)
    return wide[pl.ds(part, TB, stride=parts), :]


def other(index, step, size):
    if size & (size - 1) == 0:
        return index ^ step
    return (index + step) % size


def back(index, step, size):
    if size & (size - 1) == 0:
        return index ^ step
    return (index + size - step) % size


class Plan:
    def __init__(self, parts, owners, owned, tiles):
        self.parts, self.owners, self.owned, self.tiles = parts, owners, owned, tiles
        self.sub_len = owned // parts
        self.room = (self.sub_len + owners - 1) // owners
        self.far = 4 if owners % 4 == 0 and owners > 4 else 1
        self.near = owners // self.far
        self.chunks = [self.far - 1] + list(range(1, self.far - 1)) + [0] if self.far > 1 else [0]
        self.per_chunk = self.near * self.room
        self.pad = (self.room + 7) // 8 * 8
        self.height = self.room * TB + self.pad

    def pattern(self, k, q):
        pairs = []
        for i in range(self.owners):
            far, near = divmod(i, self.near)
            pairs.append((i, other(far, k, self.far) * self.near + other(near, q, self.near)))
        return pairs

    def source(self, me, k, q):
        return back(me // self.near, k, self.far) * self.near + back(me % self.near, q, self.near)


def step_between(here, there, size):
    if size & (size - 1) == 0:
        return here ^ there
    return lax.rem(there + size - here, size)


def fill_order(part, plan, table, order, count):
    me = lax.axis_index("shard")
    entries = plan.owners * plan.room

    def clear(j, carry):
        order[part * entries + j] = 0
        return carry

    def zero(j, carry):
        count[j] = 0
        return carry

    def enter(t, carry):
        owner = table[me, part * plan.sub_len + t] // plan.owned
        rank = count[owner]
        count[owner] = rank + 1
        k = step_between(me // plan.near, owner // plan.near, plan.far)
        q = step_between(me % plan.near, owner % plan.near, plan.near)
        order[part * entries + (k * plan.near + q) * plan.room + rank] = t
        return carry

    if entries != plan.sub_len:
        lax.fori_loop(0, entries, clear, 0)
    lax.fori_loop(0, plan.owners, zero, 0, unroll=True)
    lax.fori_loop(0, plan.sub_len, enter, 0, unroll=4)


def pack_kernel(plan, chunk, shift, lead, loads, *refs):
    parts, entries = plan.parts, plan.per_chunk
    part = lax.rem(lax.axis_index("dp") + shift, parts)
    base = part * plan.owners * plan.room + chunk * entries
    if lead:
        table, source = refs[:2]
        order, out, grads, wide, rows, count, sems = refs[2:]
        copies = [pltpu.make_async_copy(table, rows, sems.at[0]), pltpu.make_async_copy(source, grads, sems.at[1])]
    else:
        order, grads = refs[:2]
        sources, out = refs[2 : 2 + loads], refs[2 + loads]
        targets, wide = refs[3 + loads : 3 + 2 * loads], refs[3 + 2 * loads]
        copies = [pltpu.make_async_copy(a, b, refs[-1].at[n]) for n, (a, b) in enumerate(zip(sources, targets))]
    for copy in copies:
        copy.start()
    if lead:
        copies[0].wait()
        fill_order(part, plan, rows, order, count)
        copies[1].wait()

    def body(i, carry):
        out[i] = extract(grads.at[order[base + i]], wide, part, parts).astype(out.dtype)
        return carry

    lax.fori_loop(0, entries, body, 0)
    if lead:
        for s in range(1, parts):
            fill_order(lax.rem(part + s, parts), plan, rows, order, count)
    else:
        for copy in copies:
            copy.wait()


def adam_kernel(plan, chunk, first, *refs):
    parts, entries, room = plan.parts, plan.per_chunk, plan.room
    order, grads, master, moment, second = refs[:5]
    arrived = refs[5 : 4 + parts]
    refs = refs[4 + parts + (0 if first else 3) :]
    master_out, moment_out, second_out = refs[:3]
    blocks = refs[3 : 3 + plan.near]
    wide, peak = refs[3 + plan.near :]
    part = lax.axis_index("dp")
    base = part * plan.owners * room + chunk * entries
    first_fix = 1.0 / (1.0 - beta_first**step_count)
    second_fix = 1.0 / (1.0 - beta_second**step_count)
    rows = 32

    def update(i, carry):
        tile = order[base + i]
        wide[...] = grads[tile].astype(jnp.float32)
        top = None
        for b in range(0, TB, rows):
            at = pl.ds(b, rows)
            grad = wide[pl.ds(b * parts + part, rows, stride=parts), :]
            for ref in arrived:
                grad = grad + ref[i, at, :].astype(jnp.float32)
            moment_new = beta_first * moment[tile, at, :] + (1.0 - beta_first) * grad
            second_new = beta_second * second[tile, at, :] + (1.0 - beta_second) * grad * grad
            old = master[tile, at, :]
            step = moment_new * first_fix / (jnp.sqrt(second_new * second_fix) + adam_epsilon)
            master_new = old - learning_rate * (step + weight_decay * old)
            master_out[tile, at, :] = master_new
            moment_out[tile, at, :] = moment_new
            second_out[tile, at, :] = second_new
            size = jnp.abs(master_new)
            for s in range(0, rows, 8):
                top = size[s : s + 8] if top is None else jnp.maximum(top, size[s : s + 8])
        peak[i] = top
        return carry

    lax.fori_loop(0, entries, update, 0, unroll=UNROLL)
    largest = jnp.max(jnp.max(peak[...], axis=2, keepdims=True), axis=1, keepdims=True)
    rounded = (largest + scale_epsilon).astype(jnp.bfloat16).astype(jnp.float32)
    peak[...] = jnp.broadcast_to(rounded, peak.shape)
    row = lax.broadcasted_iota(jnp.int32, (plan.pad, LANES), 0)
    for q, block in enumerate(blocks):
        tail = jnp.zeros((plan.pad, LANES), jnp.float32)
        for r in range(room):
            i = q * room + r
            tile = order[base + i]
            scale = peak[i]
            inverse = 1.0 / scale
            tail = jnp.where(row == r, jnp.concatenate([scale] * (plan.pad // 8), axis=0), tail)
            for b in range(0, TB, 16):
                pair = [master_out[tile, pl.ds(b + s, 8), :] * inverse for s in (0, 8)]
                block[pl.ds(r * TB + b, 16), :] = jnp.concatenate(pair, axis=0).astype(block.dtype)
        block[pl.ds(room * TB, plan.pad), :] = tail.astype(block.dtype)


def slots_kernel(plan, table, out):
    me = lax.axis_index("shard")
    owned, sub_len = plan.owned, plan.sub_len
    local = table[...] - me * owned
    mine = (local >= 0) & (local < owned)
    before = lax.broadcasted_iota(jnp.int32, (owned, owned), 0)
    after = lax.broadcasted_iota(jnp.int32, (owned, owned), 1)
    same = before // sub_len == after // sub_len
    counts = jnp.where((before < after) & same, 1.0, 0.0).astype(jnp.bfloat16)
    flags = jnp.where(mine, 1.0, 0.0).astype(jnp.bfloat16)
    rank = jnp.dot(flags, counts, preferred_element_type=jnp.float32)
    column = lax.broadcasted_iota(jnp.int32, local.shape, 1) // sub_len
    lane = lax.broadcasted_iota(jnp.int32, out.shape, 1)
    value = jnp.where(mine, local + 1, 0).astype(jnp.float32)
    total = jnp.zeros(out.shape, jnp.float32)
    for part in range(plan.parts):
        for r in range(plan.room):
            chosen = jnp.where((column == part) & (rank == float(r)), value, 0.0)
            found = jnp.sum(chosen, axis=1, keepdims=True)
            total = jnp.where(lane == part * plan.room + r, found, total)
    out[...] = total.astype(jnp.int32) - 1


def store_kernel(*refs):
    sems = refs[-1]
    count = (len(refs) - 1) // 2
    copies = [pltpu.make_async_copy(refs[n], refs[count + n], sems.at[n]) for n in range(count)]
    for copy in copies:
        copy.start()
    for copy in copies:
        copy.wait()


def place_kernel(plan, sources, count, first, *refs):
    room = plan.room
    slots, blocks = refs[0], refs[1 : 1 + count]
    if first:
        tiles_out, scales_out, sems = refs[1 + count :]
    else:
        scales_in, _, tiles_out, scales_out, sems = refs[1 + count :]
    here, me = lax.axis_index("dp"), lax.axis_index("shard")
    lane = lax.broadcasted_iota(jnp.int32, scales_out.shape, 1)
    total = jnp.zeros(scales_out.shape, jnp.float32) if first else scales_in[...]
    entries, views = [], []
    for n, (ref, k, q, shift, at) in enumerate(sources):
        views.append(blocks[ref] if at is None else blocks[ref].at[at])
        part = lax.rem(here + plan.parts - shift, plan.parts)
        row = plan.source(me, k, q)
        for r in range(room):
            slot = slots[row, part * room + r]
            copy = pltpu.make_async_copy(views[n].at[pl.ds(r * TB, TB)], tiles_out.at[slot], sems.at[n * room + r])
            entries.append((slot, copy))
            if room * plan.owners == plan.sub_len:
                copy.start()
            else:
                pl.when(slot >= 0)(copy.start)
    for n in range(len(views)):
        tail = views[n][pl.ds(room * TB, plan.pad), :].astype(jnp.float32)
        for r in range(room):
            wide = jnp.concatenate([tail[r : r + 1]] * (scales_out.shape[1] // LANES), axis=1)
            total = jnp.where(lane == entries[n * room + r][0], wide, total)
    scales_out[...] = total
    for slot, copy in entries:
        if room * plan.owners == plan.sub_len:
            copy.wait()
        else:
            pl.when(slot >= 0)(copy.wait)


def per_device(gradients, tile_table, master, moment, second):
    owners = lax.axis_size("shard")
    parts = lax.axis_size("dp")
    owned = tile_table.shape[1]
    tiles = master.size // (TB * TB)
    plan = Plan(parts, owners, owned, tiles)
    room, entries = plan.room, plan.per_chunk

    slots = pl.pallas_call(
        functools.partial(slots_kernel, plan),
        out_shape=jax.ShapeDtypeStruct((owners, (parts * room + LANES - 1) // LANES * LANES), jnp.int32),
        in_specs=[VMEM],
        out_specs=VMEM,
        compiler_params=pltpu.CompilerParams(vmem_limit_bytes=2 << 20),
        cost_estimate=pl.CostEstimate(flops=5000000, bytes_accessed=2 << 20, transcendentals=0),
        name="slots",
    )(*in_hbm([tile_table]))

    grads = gradients.reshape(parts, tiles, TB, TB).transpose(1, 2, 0, 3).reshape(tiles, TB * parts, TB)
    states = [a.reshape(tiles, TB, TB) for a in (master, moment, second)]
    cycles = {s: [(d, (d + s) % parts) for d in range(parts)] for s in range(1, parts)}
    f32_tiles = pltpu.VMEM((tiles, TB, TB), jnp.float32)
    block_shape = pltpu.VMEM((plan.height, TB), jnp.bfloat16)

    order = None
    waiting = list(states)
    states = []
    arrived = {}
    calls = [(k, s) for k in plan.chunks for s in range(1, parts)]
    packed_shape = pltpu.VMEM((entries, TB, TB), jnp.bfloat16)
    wide_shape = pltpu.VMEM((TB * parts, TB), jnp.float32)
    for n, (k, s) in enumerate(calls):
        lead = n == 0
        loading = [] if lead else waiting[: len(waiting) if n == len(calls) - 1 else 1]
        if lead:
            operands = in_hbm([tile_table, grads])
            in_specs, out_specs = [HBM, HBM], [SMEM, VMEM, VMEM]
            out_shape = [
                jax.ShapeDtypeStruct((parts * room * owners,), jnp.int32),
                packed_shape,
                pltpu.VMEM(grads.shape, grads.dtype),
            ]
            scratch = [
                wide_shape,
                pltpu.SMEM(tile_table.shape, jnp.int32),
                pltpu.SMEM((owners,), jnp.int32),
                pltpu.SemaphoreType.DMA((2,)),
            ]
        else:
            operands = [order, *in_vmem([grads]), *in_hbm(loading)]
            in_specs, out_specs = [SMEM, VMEM] + [HBM] * len(loading), [VMEM] * (1 + len(loading))
            out_shape = [packed_shape] + [f32_tiles] * len(loading)
            scratch = [wide_shape] + [pltpu.SemaphoreType.DMA((len(loading),))] * bool(loading)
        result = pl.pallas_call(
            functools.partial(pack_kernel, plan, k, s, lead, len(loading)),
            out_shape=out_shape,
            in_specs=in_specs,
            out_specs=out_specs,
            scratch_shapes=scratch,
            compiler_params=pltpu.CompilerParams(vmem_limit_bytes=PACK_MIB << 20),
            cost_estimate=pl.CostEstimate(flops=6000000, bytes_accessed=2 << 20, transcendentals=0),
        )(*operands)
        if lead:
            order, packed, grads = result
        else:
            packed = result[0]
            states += result[1:]
            waiting = waiting[len(loading) :]
        arrived.setdefault(k, []).append(lax.ppermute(packed, "dp", cycles[s]))
    states += waiting

    news = []
    groups = {}
    for k in plan.chunks:
        count = 5 + parts - 1
        results = pl.pallas_call(
            functools.partial(adam_kernel, plan, k, not news),
            out_shape=[f32_tiles] * 3 + [block_shape] * plan.near,
            in_specs=[SMEM] + [VMEM] * (3 + parts) + [VMEM] * len(news),
            out_specs=[VMEM] * (3 + plan.near),
            input_output_aliases={count + j: j for j in range(len(news))},
            scratch_shapes=[pltpu.VMEM((TB * parts, TB), jnp.float32), pltpu.VMEM((entries, 8, LANES), jnp.float32)],
            compiler_params=pltpu.CompilerParams(vmem_limit_bytes=ADAM_MIB << 20),
            cost_estimate=pl.CostEstimate(flops=25000000, bytes_accessed=6 << 20, transcendentals=0),
        )(order, *in_vmem([grads, *states]), *arrived[k], *in_vmem(news))
        news, blocks = results[:3], results[3:]
        groups[k] = []
        for q, block in enumerate(blocks):
            if k or q:
                block = lax.ppermute(block, "shard", plan.pattern(k, q))
            groups[k].append(block)

    entries = []
    if parts == 2:
        for k in plan.chunks:
            for q, block in enumerate(groups[k]):
                passed = lax.ppermute(block, "dp", cycles[1])
                entries += [((k, q, 0, None), block), ((k, q, 1, None), passed)]
        late_chunk = plan.chunks[-2 % len(plan.chunks)]
        is_late = [key[0] == late_chunk and key[1] >= plan.near // 2 and key[2] for key, _ in entries]
    else:
        keys = [(k, q) for k in plan.chunks for q in range(plan.near)]
        stacked = jnp.stack([block for k in plan.chunks for block in groups[k]])
        for s in range(parts):
            passed = lax.ppermute(stacked, "dp", cycles[s]) if s else stacked
            entries.append(([(k, q, s, n) for n, (k, q) in enumerate(keys)], passed))
        is_late = [n == len(entries) - 1 for n in range(len(entries))]
    early = [e for e, flag in zip(entries, is_late) if not flag]
    late = [e for e, flag in zip(entries, is_late) if flag]

    news = pl.pallas_call(
        store_kernel,
        out_shape=[pltpu.HBM((tiles, TB, TB), jnp.float32)] * 3,
        in_specs=[VMEM] * 3,
        out_specs=[HBM] * 3,
        scratch_shapes=[pltpu.SemaphoreType.DMA((3,))],
        compiler_params=pltpu.CompilerParams(vmem_limit_bytes=1 << 20),
        cost_estimate=pl.CostEstimate(flops=5000000, bytes_accessed=2 << 20, transcendentals=0),
        name="store",
    )(*in_vmem(news))

    tiles_shape = pltpu.HBM((owned, TB, TB), jnp.bfloat16)
    width = (owned + LANES - 1) // LANES * LANES

    def place(group, previous):
        count = 1 + len(group)
        sources = []
        for n, (key, _) in enumerate(group):
            sources += [(n, *each) for each in (key if isinstance(key, list) else [key])]
        return pl.pallas_call(
            functools.partial(place_kernel, plan, sources, len(group), not previous),
            out_shape=[tiles_shape, jax.ShapeDtypeStruct((1, width), jnp.float32)],
            in_specs=[SMEM] + [VMEM] * len(group) + ([VMEM, HBM] if previous else []),
            out_specs=[HBM, VMEM],
            input_output_aliases={count + 1: 0} if previous else {},
            scratch_shapes=[pltpu.SemaphoreType.DMA((len(sources) * room,))],
            compiler_params=pltpu.CompilerParams(vmem_limit_bytes=24 << 20),
            cost_estimate=pl.CostEstimate(flops=5000000, bytes_accessed=2 << 20, transcendentals=0),
        )(slots, *[a for _, a in group], *([previous[1], *in_hbm([previous[0]])] if previous else []))

    placed = place(early, None)
    tiles_out, scales = place(late, placed)
    scales_out = scales[0, :owned].astype(jnp.bfloat16)
    return (*[a.reshape(master.shape) for a in news], tiles_out, scales_out)


def solution(mesh):
    in_specs = (
        P("dp", "shard", None, None),
        P(),
        P("shard", "dp", None),
        P("shard", "dp", None),
        P("shard", "dp", None),
    )
    out_specs = (
        P("shard", "dp", None),
        P("shard", "dp", None),
        P("shard", "dp", None),
        P("shard", None, None),
        P("shard"),
    )

    return jax.shard_map(per_device, mesh=mesh, in_specs=in_specs, out_specs=out_specs, check_vma=False)
```

```python
import functools

import jax
import jax.numpy as jnp
from jax import lax
from jax.experimental import pallas as pl
from jax.experimental.pallas import tpu as pltpu
from jax.sharding import PartitionSpec as P


TB = 128
LANES = 128
UNROLL = 2
SPLIT = 4
STAGES = {(0, 2, 1): 2, (0, 3, 1): 2, (0, 2, 0): 1, (0, 3, 0): 1, (0, 1, 1): 1}
STAGES |= {(k, q, s): 1 for k in (1, 2) for q in range(4) for s in range(2)}
PACK_MIB = 4
ADAM_MIB = 4


beta_first = 0.9
beta_second = 0.95
learning_rate = 0.002
weight_decay = 0.1
adam_epsilon = 1e-08
scale_epsilon = 1e-06
step_count = 10

HBM = pl.BlockSpec(memory_space=pltpu.HBM)
VMEM = pl.BlockSpec(memory_space=pltpu.VMEM)
SMEM = pl.BlockSpec(memory_space=pltpu.SMEM)


def in_hbm(arrays):
    return [pltpu.with_memory_space_constraint(a, pltpu.HBM) for a in arrays]


def in_vmem(arrays):
    return [pltpu.with_memory_space_constraint(a, pltpu.VMEM) for a in arrays]


def extract(raw, wide, part, parts):
    wide[...] = raw[...].astype(jnp.float32)
    return wide[pl.ds(part, TB, stride=parts), :]


def other(index, step, size):
    if size & (size - 1) == 0:
        return index ^ step
    return (index + step) % size


def back(index, step, size):
    if size & (size - 1) == 0:
        return index ^ step
    return (index + size - step) % size


class Plan:
    def __init__(self, parts, owners, owned, tiles):
        self.parts, self.owners, self.owned, self.tiles = parts, owners, owned, tiles
        self.sub_len = owned // parts
        self.room = (self.sub_len + owners - 1) // owners
        self.far = 4 if owners % 4 == 0 and owners > 4 else 1
        self.near = owners // self.far
        self.chunks = [self.far - 1] + list(range(1, self.far - 1)) + [0] if self.far > 1 else [0]
        self.per_chunk = self.near * self.room
        self.pad = (self.room + 7) // 8 * 8
        self.height = self.room * TB + self.pad

    def pattern(self, k, q):
        pairs = []
        for i in range(self.owners):
            far, near = divmod(i, self.near)
            pairs.append((i, other(far, k, self.far) * self.near + other(near, q, self.near)))
        return pairs

    def source(self, me, k, q):
        return back(me // self.near, k, self.far) * self.near + back(me % self.near, q, self.near)


def step_between(here, there, size):
    if size & (size - 1) == 0:
        return here ^ there
    return lax.rem(there + size - here, size)


def fill_order(part, plan, table, order, base, count):
    me = lax.axis_index("shard")
    entries = plan.owners * plan.room

    def clear(j, carry):
        order[base + j] = 0
        return carry

    def zero(j, carry):
        count[j] = 0
        return carry

    def enter(t, carry):
        owner = table[me, part * plan.sub_len + t] // plan.owned
        rank = count[owner]
        count[owner] = rank + 1
        k = step_between(me // plan.near, owner // plan.near, plan.far)
        q = step_between(me % plan.near, owner % plan.near, plan.near)
        order[base + (k * plan.near + q) * plan.room + rank] = t
        return carry

    if entries != plan.sub_len:
        lax.fori_loop(0, entries, clear, 0)
    lax.fori_loop(0, plan.owners, zero, 0, unroll=True)
    lax.fori_loop(0, plan.sub_len, enter, 0, unroll=4)


def find_slots(plan, table, out):
    me = lax.axis_index("shard")
    owned, sub_len = plan.owned, plan.sub_len
    local = table[...] - me * owned
    mine = (local >= 0) & (local < owned)
    before = lax.broadcasted_iota(jnp.int32, (owned, owned), 0)
    after = lax.broadcasted_iota(jnp.int32, (owned, owned), 1)
    same = before // sub_len == after // sub_len
    counts = jnp.where((before < after) & same, 1.0, 0.0).astype(jnp.bfloat16)
    flags = jnp.where(mine, 1.0, 0.0).astype(jnp.bfloat16)
    rank = jnp.dot(flags, counts, preferred_element_type=jnp.float32)
    column = lax.broadcasted_iota(jnp.int32, local.shape, 1) // sub_len
    lane = lax.broadcasted_iota(jnp.int32, out.shape, 1)
    value = jnp.where(mine, local + 1, 0).astype(jnp.float32)
    total = jnp.zeros(out.shape, jnp.float32)
    for part in range(plan.parts):
        for r in range(plan.room):
            chosen = jnp.where((column == part) & (rank == float(r)), value, 0.0)
            found = jnp.sum(chosen, axis=1, keepdims=True)
            total = jnp.where(lane == part * plan.room + r, found, total)
    out[...] = total.astype(jnp.int32) - 1


def pack_kernel(plan, chunk, shift, lead, own, loads, *refs):
    parts, entries, room = plan.parts, plan.per_chunk, plan.room
    here = lax.axis_index("dp")
    part = lax.rem(here + shift, parts)
    refs = list(refs)
    take = lambda n: [refs.pop(0) for _ in range(n)]
    (table,) = take(1) if lead or own else (None,)
    (order,) = take(1) if not lead else (None,)
    (grads,) = take(1) if not lead else (None,)
    sources = take(loads)
    (order,) = take(1) if lead else (order,)
    (out,) = take(1)
    (order_own, slots) = take(2) if own else (None, None)
    targets = take(loads)
    if lead:
        grads = targets[0]
    (wide,) = take(1)
    rows, count = take(2) if lead or own else (None, None)
    (flat,) = take(1) if own else (None,)
    (sems,) = take(1)
    pairs = list(zip(sources, targets))
    pairs += [(table, rows)] * bool(lead or own) + [(table, flat)] * bool(own)
    copies = [pltpu.make_async_copy(a, b, sems.at[n]) for n, (a, b) in enumerate(pairs)]
    for copy in copies:
        copy.start()
    entries_of_part = plan.owners * room
    if lead:
        copies[loads].wait()
        fill_order(part, plan, rows, order, part * entries_of_part, count)
        copies[0].wait()
    base = part * entries_of_part + chunk * entries

    def body(i, carry):
        out[i] = extract(grads.at[order[base + i]], wide, part, parts).astype(out.dtype)
        return carry

    lax.fori_loop(0, entries, body, 0)
    if lead:
        for s in range(1, parts - 1):
            later = lax.rem(part + s, parts)
            fill_order(later, plan, rows, order, later * entries_of_part, count)
    if own:
        if not lead:
            copies[loads].wait()
        copies[loads + 1].wait()
        fill_order(here, plan, rows, order_own, 0, count)
        find_slots(plan, flat, slots)
    for n, copy in enumerate(copies):
        if not (lead and n == 0) and not (lead and n == loads) and not (own and n >= loads):
            copy.wait()


def adam_kernel(plan, chunk, first, *refs):
    parts, entries, room = plan.parts, plan.per_chunk, plan.room
    order, grads, master, moment, second = refs[:5]
    arrived = refs[5 : 4 + parts]
    refs = refs[4 + parts + (0 if first else 3) :]
    master_out, moment_out, second_out = refs[:3]
    blocks = refs[3 : 3 + plan.near]
    wide, peak = refs[3 + plan.near :]
    part = lax.axis_index("dp")
    base = chunk * entries
    first_fix = 1.0 / (1.0 - beta_first**step_count)
    second_fix = 1.0 / (1.0 - beta_second**step_count)
    rows = 32

    def update(i, carry):
        tile = order[base + i]
        wide[...] = grads[tile].astype(jnp.float32)
        top = None
        for b in range(0, TB, rows):
            at = pl.ds(b, rows)
            grad = wide[pl.ds(b * parts + part, rows, stride=parts), :]
            for ref in arrived:
                grad = grad + ref[i, at, :].astype(jnp.float32)
            moment_new = beta_first * moment[tile, at, :] + (1.0 - beta_first) * grad
            second_new = beta_second * second[tile, at, :] + (1.0 - beta_second) * grad * grad
            old = master[tile, at, :]
            step = moment_new * first_fix / (jnp.sqrt(second_new * second_fix) + adam_epsilon)
            master_new = old - learning_rate * (step + weight_decay * old)
            master_out[tile, at, :] = master_new
            moment_out[tile, at, :] = moment_new
            second_out[tile, at, :] = second_new
            size = jnp.abs(master_new)
            for s in range(0, rows, 8):
                top = size[s : s + 8] if top is None else jnp.maximum(top, size[s : s + 8])
        peak[i] = top
        return carry

    lax.fori_loop(0, entries, update, 0, unroll=UNROLL)
    largest = jnp.max(jnp.max(peak[...], axis=2, keepdims=True), axis=1, keepdims=True)
    rounded = (largest + scale_epsilon).astype(jnp.bfloat16).astype(jnp.float32)
    peak[...] = jnp.broadcast_to(rounded, peak.shape)
    row = lax.broadcasted_iota(jnp.int32, (plan.pad, LANES), 0)
    for q, block in enumerate(blocks):
        tail = jnp.zeros((plan.pad, LANES), jnp.float32)
        for r in range(room):
            i = q * room + r
            tile = order[base + i]
            scale = peak[i]
            inverse = 1.0 / scale
            tail = jnp.where(row == r, jnp.concatenate([scale] * (plan.pad // 8), axis=0), tail)
            for b in range(0, TB, 16):
                pair = [master_out[tile, pl.ds(b + s, 8), :] * inverse for s in (0, 8)]
                block[pl.ds(r * TB + b, 16), :] = jnp.concatenate(pair, axis=0).astype(block.dtype)
        block[pl.ds(room * TB, plan.pad), :] = tail.astype(block.dtype)


def tails_kernel(plan, *refs):
    out = refs[-1]
    for n, ref in enumerate(refs[:-1]):
        out[n] = ref[pl.ds(plan.room * TB, plan.pad), :]


def place_kernel(plan, sources, count, tails, first, gathers, *refs):
    room = plan.room
    refs = list(refs)
    take = lambda n: [refs.pop(0) for _ in range(n)]
    (slots,), blocks = take(1), take(count)
    late = take(1) if tails else []
    held = take(3) if first else []
    before = take(2)[1:] if gathers and not first else []
    if not first and not gathers:
        take(1)
    (tiles_out,) = take(1)
    (scales_out,) = take(1) if gathers else (None,)
    saved = take(3) if first else []
    (sems,) = take(1)
    stores = []
    for a, b in zip(held, saved):
        for n in range(0, plan.tiles, plan.tiles // SPLIT):
            piece = pl.ds(n, plan.tiles // SPLIT)
            stores.append(pltpu.make_async_copy(a.at[piece], b.at[piece], refs[0].at[len(stores)]))
    for copy in stores:
        copy.start()
    here, me = lax.axis_index("dp"), lax.axis_index("shard")

    def slot_of(k, q, shift, r):
        part = lax.rem(here + plan.parts - shift, plan.parts)
        return slots[plan.source(me, k, q), part * room + r]

    entries, views = [], []
    for n, (ref, k, q, shift, at) in enumerate(sources):
        views.append(blocks[ref] if at is None else blocks[ref].at[at])
        for r in range(room):
            slot = slot_of(k, q, shift, r)
            copy = pltpu.make_async_copy(views[n].at[pl.ds(r * TB, TB)], tiles_out.at[slot], sems.at[n * room + r])
            entries.append((slot, copy))
            if room * plan.owners == plan.sub_len:
                copy.start()
            else:
                pl.when(slot >= 0)(copy.start)
    if gathers:
        lane = lax.broadcasted_iota(jnp.int32, scales_out.shape, 1)
        total = before[0][...] if before else jnp.zeros(scales_out.shape, jnp.float32)
        ends = [(view[pl.ds(room * TB, plan.pad), :], key[1:4]) for view, key in zip(views, sources)]
        ends += [(late[0][n], key) for n, key in enumerate(tails)]
        for rows, (k, q, shift) in ends:
            for r in range(room):
                wide = jnp.concatenate([rows[r : r + 1].astype(jnp.float32)] * (scales_out.shape[1] // LANES), axis=1)
                total = jnp.where(lane == slot_of(k, q, shift, r), wide, total)
        scales_out[...] = total
    for slot, copy in entries:
        if room * plan.owners == plan.sub_len:
            copy.wait()
        else:
            pl.when(slot >= 0)(copy.wait)
    for copy in stores:
        copy.wait()


def per_device(gradients, tile_table, master, moment, second):
    owners = lax.axis_size("shard")
    parts = lax.axis_size("dp")
    owned = tile_table.shape[1]
    tiles = master.size // (TB * TB)
    plan = Plan(parts, owners, owned, tiles)
    room, entries = plan.room, plan.per_chunk

    grads = gradients.reshape(parts, tiles, TB, TB).transpose(1, 2, 0, 3).reshape(tiles, TB * parts, TB)
    states = [a.reshape(tiles, TB, TB) for a in (master, moment, second)]
    cycles = {s: [(d, (d + s) % parts) for d in range(parts)] for s in range(1, parts)}
    f32_tiles = pltpu.VMEM((tiles, TB, TB), jnp.float32)
    block_shape = pltpu.VMEM((plan.height, TB), jnp.bfloat16)

    order = None
    waiting = list(states)
    states = []
    arrived = {}
    calls = [(k, s) for k in plan.chunks for s in range(1, parts)]
    packed_shape = pltpu.VMEM((entries, TB, TB), jnp.bfloat16)
    slots_shape = jax.ShapeDtypeStruct((owners, (parts * room + LANES - 1) // LANES * LANES), jnp.int32)
    for n, (k, s) in enumerate(calls):
        lead, own = n == 0, n == min(1, len(calls) - 1)
        loading = waiting[: len(waiting) if n == len(calls) - 1 else 1 - lead]
        waiting = waiting[len(loading) :]
        loads = len(loading) + lead
        tabled = lead or own
        operands = in_hbm([tile_table]) * tabled
        operands += in_hbm([grads]) if lead else [order, *in_vmem([grads])]
        operands += in_hbm(loading)
        out_shape = [jax.ShapeDtypeStruct((parts * room * owners,), jnp.int32)] * lead + [packed_shape]
        out_shape += [jax.ShapeDtypeStruct((room * owners,), jnp.int32), slots_shape] * own
        out_shape += [pltpu.VMEM(grads.shape, grads.dtype)] * lead + [f32_tiles] * len(loading)
        result = pl.pallas_call(
            functools.partial(pack_kernel, plan, k, s, lead, own, loads),
            out_shape=out_shape,
            in_specs=[HBM] * tabled + [SMEM, VMEM] * (not lead) + [HBM] * loads,
            out_specs=[SMEM] * lead + [VMEM] + [SMEM, VMEM] * own + [VMEM] * loads,
            scratch_shapes=[pltpu.VMEM((TB * parts, TB), jnp.float32)]
            + [pltpu.SMEM(tile_table.shape, jnp.int32), pltpu.SMEM((owners,), jnp.int32)] * tabled
            + [pltpu.VMEM(tile_table.shape, jnp.int32)] * own
            + [pltpu.SemaphoreType.DMA((max(1, loads + tabled + own),))],
            compiler_params=pltpu.CompilerParams(vmem_limit_bytes=PACK_MIB << 20),
            cost_estimate=pl.CostEstimate(flops=6000000, bytes_accessed=2 << 20, transcendentals=0),
        )(*operands)
        result = list(result)
        if lead:
            order = result.pop(0)
        packed = result.pop(0)
        if own:
            order_own, slots = result.pop(0), result.pop(0)
        if lead:
            grads = result.pop(0)
        states += result
        arrived.setdefault(k, []).append(lax.ppermute(packed, "dp", cycles[s]))

    news = []
    groups = {}
    for k in plan.chunks:
        count = 5 + parts - 1
        results = pl.pallas_call(
            functools.partial(adam_kernel, plan, k, not news),
            out_shape=[f32_tiles] * 3 + [block_shape] * plan.near,
            in_specs=[SMEM] + [VMEM] * (3 + parts) + [VMEM] * len(news),
            out_specs=[VMEM] * (3 + plan.near),
            input_output_aliases={count + j: j for j in range(len(news))},
            scratch_shapes=[pltpu.VMEM((TB * parts, TB), jnp.float32), pltpu.VMEM((entries, 8, LANES), jnp.float32)],
            compiler_params=pltpu.CompilerParams(vmem_limit_bytes=ADAM_MIB << 20),
            cost_estimate=pl.CostEstimate(flops=25000000, bytes_accessed=6 << 20, transcendentals=0),
        )(order_own, *in_vmem([grads, *states]), *arrived[k], *in_vmem(news))
        news, blocks = results[:3], results[3:]
        groups[k] = []
        for q, block in enumerate(blocks):
            if k or q:
                block = lax.ppermute(block, "shard", plan.pattern(k, q))
            groups[k].append(block)

    entries = []
    tails, tail_keys = [], []
    if parts == 2:
        for k in plan.chunks:
            for q, block in enumerate(groups[k]):
                passed = lax.ppermute(block, "dp", cycles[1])
                entries += [((k, q, 0, None), block), ((k, q, 1, None), passed)]
        stage = [STAGES.get(key[:3], 0) for key, _ in entries]
        stage = stage if 2 in stage else [2 * (n == len(entries) - 1) for n in range(len(entries))]
        tail_keys = [key[:3] for (key, _), at in zip(entries, stage) if at == 2]
        ends = pl.pallas_call(
            functools.partial(tails_kernel, plan),
            out_shape=pltpu.VMEM((len(tail_keys), plan.pad, LANES), jnp.bfloat16),
            in_specs=[VMEM] * len(tail_keys),
            out_specs=VMEM,
            compiler_params=pltpu.CompilerParams(vmem_limit_bytes=1 << 20),
            cost_estimate=pl.CostEstimate(flops=1000000, bytes_accessed=1 << 20, transcendentals=0),
            name="tails",
        )(*[groups[k][q] for k, q, _ in tail_keys])
        tails = [lax.ppermute(ends, "dp", cycles[1])]
    else:
        keys = [(k, q) for k in plan.chunks for q in range(plan.near)]
        stacked = jnp.stack([block for k in plan.chunks for block in groups[k]])
        for s in range(parts):
            passed = lax.ppermute(stacked, "dp", cycles[s]) if s else stacked
            entries.append(([(k, q, s, n) for n, (k, q) in enumerate(keys)], passed))
        stage = [0] * len(entries)
    tiles_shape = pltpu.HBM((owned, TB, TB), jnp.bfloat16)
    width = (owned + LANES - 1) // LANES * LANES

    def place(at, previous, ends):
        group = [e for e, level in zip(entries, stage) if level == at]
        first, gathers = not previous, at < 2
        sources = []
        for n, (key, _) in enumerate(group):
            sources += [(n, *each) for each in (key if isinstance(key, list) else [key])]
        operands = [slots, *[a for _, a in group], *ends]
        operands += in_vmem(news) if first else in_hbm(previous[:1])
        operands += previous[1:] if gathers else []
        return pl.pallas_call(
            functools.partial(place_kernel, plan, sources, len(group), tail_keys if ends else [], first, gathers),
            out_shape=[tiles_shape]
            + [jax.ShapeDtypeStruct((1, width), jnp.float32)] * gathers
            + [pltpu.HBM((tiles, TB, TB), jnp.float32)] * (3 * first),
            in_specs=[SMEM]
            + [VMEM] * (len(group) + len(ends))
            + ([VMEM] * 3 if first else [HBM] + [VMEM] * gathers),
            out_specs=[HBM] + [VMEM] * gathers + [HBM] * (3 * first),
            input_output_aliases={} if first else {1 + len(group) + len(ends): 0},
            scratch_shapes=[pltpu.SemaphoreType.DMA((len(sources) * room,))]
            + [pltpu.SemaphoreType.DMA((3 * SPLIT,))] * first,
            compiler_params=pltpu.CompilerParams(vmem_limit_bytes=24 << 20),
            cost_estimate=pl.CostEstimate(flops=5000000, bytes_accessed=2 << 20, transcendentals=0),
        )(*operands)

    staged = max(stage) > 0
    tiles_out, scales, *news = place(0, [], [] if 1 in stage else tails)
    if 1 in stage:
        tiles_out, scales = place(1, [tiles_out, scales], tails)
    scales_out = scales[0, :owned].astype(jnp.bfloat16)
    if staged:
        (tiles_out,) = place(2, [tiles_out], [])
    return (*[a.reshape(master.shape) for a in news], tiles_out, scales_out)


def solution(mesh):
    in_specs = (
        P("dp", "shard", None, None),
        P(),
        P("shard", "dp", None),
        P("shard", "dp", None),
        P("shard", "dp", None),
    )
    out_specs = (
        P("shard", "dp", None),
        P("shard", "dp", None),
        P("shard", "dp", None),
        P("shard", None, None),
        P("shard"),
    )

    return jax.shard_map(per_device, mesh=mesh, in_specs=in_specs, out_specs=out_specs, check_vma=False)
```

```python
import functools

import jax
import jax.numpy as jnp
from jax import lax
from jax.experimental import pallas as pl
from jax.experimental.pallas import tpu as pltpu
from jax.sharding import PartitionSpec as P


TB = 128
LANES = 128
UNROLL = 2
SPLIT = 4
MERGES = (
    ((3, 0), (3, 1), (3, 2), (3, 3)),
    ((1, 0), (1, 1), (1, 2), (1, 3)),
    ((2, 0),),
    ((2, 1), (0, 1)),
    ((2, 2), (2, 3)),
    ((0, 2), (0, 3)),
)
PACK_MIB = 4
ADAM_MIB = 4


beta_first = 0.9
beta_second = 0.95
learning_rate = 0.002
weight_decay = 0.1
adam_epsilon = 1e-08
scale_epsilon = 1e-06
step_count = 10

HBM = pl.BlockSpec(memory_space=pltpu.HBM)
VMEM = pl.BlockSpec(memory_space=pltpu.VMEM)
SMEM = pl.BlockSpec(memory_space=pltpu.SMEM)


def in_hbm(arrays):
    return [pltpu.with_memory_space_constraint(a, pltpu.HBM) for a in arrays]


def in_vmem(arrays):
    return [pltpu.with_memory_space_constraint(a, pltpu.VMEM) for a in arrays]


def extract(raw, wide, part, parts):
    wide[...] = raw[...].astype(jnp.float32)
    return wide[pl.ds(part, TB, stride=parts), :]


def other(index, step, size):
    if size & (size - 1) == 0:
        return index ^ step
    return (index + step) % size


def back(index, step, size):
    if size & (size - 1) == 0:
        return index ^ step
    return (index + size - step) % size


class Plan:
    def __init__(self, parts, owners, owned, tiles):
        self.parts, self.owners, self.owned, self.tiles = parts, owners, owned, tiles
        self.sub_len = owned // parts
        self.room = (self.sub_len + owners - 1) // owners
        self.far = 4 if owners % 4 == 0 and owners > 4 else 1
        self.near = owners // self.far
        self.chunks = [self.far - 1] + list(range(1, self.far - 1)) + [0] if self.far > 1 else [0]
        self.per_chunk = self.near * self.room
        self.pad = (self.room + 7) // 8 * 8
        self.height = self.room * TB + self.pad

    def pattern(self, k, q):
        pairs = []
        for i in range(self.owners):
            far, near = divmod(i, self.near)
            pairs.append((i, other(far, k, self.far) * self.near + other(near, q, self.near)))
        return pairs

    def source(self, me, k, q):
        return back(me // self.near, k, self.far) * self.near + back(me % self.near, q, self.near)


def step_between(here, there, size):
    if size & (size - 1) == 0:
        return here ^ there
    return lax.rem(there + size - here, size)


def fill_order(part, plan, table, order, base, count):
    me = lax.axis_index("shard")
    entries = plan.owners * plan.room

    def clear(j, carry):
        order[base + j] = 0
        return carry

    def zero(j, carry):
        count[j] = 0
        return carry

    def enter(t, carry):
        owner = table[me, part * plan.sub_len + t] // plan.owned
        rank = count[owner]
        count[owner] = rank + 1
        k = step_between(me // plan.near, owner // plan.near, plan.far)
        q = step_between(me % plan.near, owner % plan.near, plan.near)
        order[base + (k * plan.near + q) * plan.room + rank] = t
        return carry

    if entries != plan.sub_len:
        lax.fori_loop(0, entries, clear, 0)
    lax.fori_loop(0, plan.owners, zero, 0, unroll=True)
    lax.fori_loop(0, plan.sub_len, enter, 0, unroll=12)


def find_slots(plan, table, out):
    me = lax.axis_index("shard")
    owned, sub_len = plan.owned, plan.sub_len
    local = table[...] - me * owned
    mine = (local >= 0) & (local < owned)
    before = lax.broadcasted_iota(jnp.int32, (owned, owned), 0)
    after = lax.broadcasted_iota(jnp.int32, (owned, owned), 1)
    same = before // sub_len == after // sub_len
    counts = jnp.where((before < after) & same, 1.0, 0.0).astype(jnp.bfloat16)
    flags = jnp.where(mine, 1.0, 0.0).astype(jnp.bfloat16)
    rank = jnp.dot(flags, counts, preferred_element_type=jnp.float32)
    column = lax.broadcasted_iota(jnp.int32, local.shape, 1) // sub_len
    lane = lax.broadcasted_iota(jnp.int32, out.shape, 1)
    value = jnp.where(mine, local + 1, 0).astype(jnp.float32)
    total = jnp.zeros(out.shape, jnp.float32)
    for part in range(plan.parts):
        for r in range(plan.room):
            chosen = jnp.where((column == part) & (rank == float(r)), value, 0.0)
            found = jnp.sum(chosen, axis=1, keepdims=True)
            total = jnp.where(lane == part * plan.room + r, found, total)
    out[...] = total.astype(jnp.int32) - 1


def pack_kernel(plan, chunk, shift, lead, own, loads, *refs):
    parts, entries, room = plan.parts, plan.per_chunk, plan.room
    here = lax.axis_index("dp")
    part = lax.rem(here + shift, parts)
    refs = list(refs)
    take = lambda n: [refs.pop(0) for _ in range(n)]
    (table,) = take(1) if lead or own else (None,)
    (order,) = take(1) if not lead else (None,)
    (grads,) = take(1) if not lead else (None,)
    sources = take(loads)
    (order,) = take(1) if lead else (order,)
    (out,) = take(1)
    (order_own, slots) = take(2) if own else (None, None)
    targets = take(loads)
    if lead:
        grads = targets[0]
    (wide,) = take(1)
    rows, count = take(2) if lead or own else (None, None)
    (flat,) = take(1) if own else (None,)
    (sems,) = take(1)
    pairs = []
    for a, b in zip(sources, targets):
        size = a.shape[0] // SPLIT
        pairs += [(a.at[pl.ds(n * size, size)], b.at[pl.ds(n * size, size)]) for n in range(SPLIT)]
    loads *= SPLIT
    pairs += [(table, rows)] * bool(lead or own) + [(table, flat)] * bool(own)
    copies = [pltpu.make_async_copy(a, b, sems.at[n]) for n, (a, b) in enumerate(pairs)]
    for copy in copies:
        copy.start()
    entries_of_part = plan.owners * room
    if lead:
        copies[loads].wait()
        fill_order(part, plan, rows, order, part * entries_of_part, count)
        for copy in copies[:loads]:
            copy.wait()
    base = part * entries_of_part + chunk * entries

    def body(i, carry):
        out[i] = extract(grads.at[order[base + i]], wide, part, parts).astype(out.dtype)
        return carry

    lax.fori_loop(0, entries, body, 0, unroll=3)
    if lead:
        for s in range(1, parts - 1):
            later = lax.rem(part + s, parts)
            fill_order(later, plan, rows, order, later * entries_of_part, count)
    if own:
        if not lead:
            copies[loads].wait()
        copies[loads + 1].wait()
        fill_order(here, plan, rows, order_own, 0, count)
        find_slots(plan, flat, slots)
    for n, copy in enumerate(copies):
        if n < loads and not lead:
            copy.wait()


def adam_kernel(plan, chunk, first, *refs):
    parts, entries, room = plan.parts, plan.per_chunk, plan.room
    order, grads, master, moment, second = refs[:5]
    arrived = refs[5 : 4 + parts]
    refs = refs[4 + parts + (0 if first else 3) :]
    master_out, moment_out, second_out = refs[:3]
    blocks = refs[3 : 3 + plan.near]
    apart = refs[3 + plan.near : -2]
    wide, peak = refs[-2:]
    part = lax.axis_index("dp")
    base = chunk * entries
    first_fix = 1.0 / (1.0 - beta_first**step_count)
    second_fix = 1.0 / (1.0 - beta_second**step_count)
    rows = 32

    def update(i, carry):
        tile = order[base + i]
        wide[...] = grads[tile].astype(jnp.float32)
        top = None
        for b in range(0, TB, rows):
            at = pl.ds(b, rows)
            grad = wide[pl.ds(b * parts + part, rows, stride=parts), :]
            for ref in arrived:
                grad = grad + ref[i, at, :].astype(jnp.float32)
            moment_new = beta_first * moment[tile, at, :] + (1.0 - beta_first) * grad
            second_new = beta_second * second[tile, at, :] + (1.0 - beta_second) * grad * grad
            old = master[tile, at, :]
            step = moment_new * first_fix / (jnp.sqrt(second_new * second_fix) + adam_epsilon)
            master_new = old - learning_rate * (step + weight_decay * old)
            master_out[tile, at, :] = master_new
            moment_out[tile, at, :] = moment_new
            second_out[tile, at, :] = second_new
            size = jnp.abs(master_new)
            for s in range(0, rows, 8):
                top = size[s : s + 8] if top is None else jnp.maximum(top, size[s : s + 8])
        peak[i] = top
        return carry

    lax.fori_loop(0, entries, update, 0, unroll=UNROLL)
    largest = jnp.max(jnp.max(peak[...], axis=2, keepdims=True), axis=1, keepdims=True)
    rounded = (largest + scale_epsilon).astype(jnp.bfloat16).astype(jnp.float32)
    peak[...] = jnp.broadcast_to(rounded, peak.shape)
    row = lax.broadcasted_iota(jnp.int32, (plan.pad, LANES), 0)
    for q, block in enumerate(blocks):
        tail = jnp.zeros((plan.pad, LANES), jnp.float32)
        for r in range(room):
            i = q * room + r
            tile = order[base + i]
            scale = peak[i]
            inverse = 1.0 / scale
            tail = jnp.where(row == r, jnp.concatenate([scale] * (plan.pad // 8), axis=0), tail)
            for b in range(0, TB, 16):
                pair = [master_out[tile, pl.ds(b + s, 8), :] * inverse for s in (0, 8)]
                block[pl.ds(r * TB + b, 16), :] = jnp.concatenate(pair, axis=0).astype(block.dtype)
        if q == 0 and apart:
            apart[0][...] = tail.astype(block.dtype)
        else:
            block[pl.ds(room * TB, plan.pad), :] = tail.astype(block.dtype)


def store_kernel(held, saved, sems):
    size = held.shape[0] // SPLIT
    copies = []
    for n in range(SPLIT):
        piece = pl.ds(n * size, size)
        copies.append(pltpu.make_async_copy(held.at[piece], saved.at[piece], sems.at[n]))
    for copy in copies:
        copy.start()
    for copy in copies:
        copy.wait()


def merge_kernel(plan, count, ends, *refs):
    blocks, tails = refs[:count], refs[count : count + ends]
    rows = plan.room * TB
    for n, block in enumerate(blocks):
        refs[count + ends][pl.ds(n * rows, rows), :] = block[pl.ds(0, rows), :]
    if ends:
        out = refs[-1]
        group = lax.broadcasted_iota(jnp.int32, out.shape, 1) // (LANES // ends)
        total = jnp.zeros(out.shape, jnp.float32)
        for n, ref in enumerate(tails):
            tail = ref[pl.ds(ref.shape[0] - plan.pad, plan.pad), :].astype(jnp.float32)
            total = jnp.where(group == n, tail, total)
        out[...] = total.astype(out.dtype)


def place_kernel(plan, sources, count, keys, first, gathers, *refs):
    room = plan.room
    refs = list(refs)
    take = lambda n: [refs.pop(0) for _ in range(n)]
    (slots,), blocks = take(1), take(count)
    late = take(plan.parts) if gathers and keys else []
    if not first:
        take(1)
    (tiles_out,) = take(1)
    (scales_out,) = take(1) if gathers else (None,)
    (sems,) = take(1)
    here, me = lax.axis_index("dp"), lax.axis_index("shard")

    def slot_of(k, q, shift, r):
        part = lax.rem(here + plan.parts - shift, plan.parts)
        return slots[plan.source(me, k, q), part * room + r]

    entries, views = [], []
    for n, (ref, k, q, shift, at) in enumerate(sources):
        stacked = len(blocks[ref].shape) == 3
        views.append(blocks[ref].at[at] if stacked else blocks[ref])
        start = 0 if stacked or at is None else at * room * TB
        for r in range(room):
            slot = slot_of(k, q, shift, r)
            copy = pltpu.make_async_copy(views[n].at[pl.ds(start + r * TB, TB)], tiles_out.at[slot], sems.at[n * room + r])
            entries.append((slot, copy))
            if room * plan.owners == plan.sub_len:
                copy.start()
            else:
                pl.when(slot >= 0)(copy.start)
    if gathers:
        lane = lax.broadcasted_iota(jnp.int32, scales_out.shape, 1)
        total = jnp.zeros(scales_out.shape, jnp.float32)
        ends = []
        if keys:
            for shift, ref in enumerate(late):
                packed = ref[...].astype(jnp.float32)
                for n, (k, q) in enumerate(keys):
                    at = n * (LANES // len(keys))
                    ends.append((jnp.broadcast_to(packed[:, at : at + 1], packed.shape), (k, q, shift)))
        else:
            ends = [(view[pl.ds(room * TB, plan.pad), :], key[1:4]) for view, key in zip(views, sources)]
        for rows, (k, q, shift) in ends:
            for r in range(room):
                wide = jnp.concatenate([rows[r : r + 1].astype(jnp.float32)] * (scales_out.shape[1] // LANES), axis=1)
                total = jnp.where(lane == slot_of(k, q, shift, r), wide, total)
        scales_out[...] = total
    for slot, copy in entries:
        if room * plan.owners == plan.sub_len:
            copy.wait()
        else:
            pl.when(slot >= 0)(copy.wait)


def per_device(gradients, tile_table, master, moment, second):
    owners = lax.axis_size("shard")
    parts = lax.axis_size("dp")
    owned = tile_table.shape[1]
    tiles = master.size // (TB * TB)
    plan = Plan(parts, owners, owned, tiles)
    room, entries = plan.room, plan.per_chunk

    grads = gradients.reshape(parts, tiles, TB, TB).transpose(1, 2, 0, 3).reshape(tiles, TB * parts, TB)
    states = [a.reshape(tiles, TB, TB) for a in (master, moment, second)]
    cycles = {s: [(d, (d + s) % parts) for d in range(parts)] for s in range(1, parts)}
    f32_tiles = pltpu.VMEM((tiles, TB, TB), jnp.float32)
    block_shape = pltpu.VMEM((plan.height, TB), jnp.bfloat16)

    order = None
    waiting = list(states)
    states = []
    arrived = {}
    calls = [(k, s) for k in plan.chunks for s in range(1, parts)]
    packed_shape = pltpu.VMEM((entries, TB, TB), jnp.bfloat16)
    slots_shape = jax.ShapeDtypeStruct((owners, (parts * room + LANES - 1) // LANES * LANES), jnp.int32)
    for n, (k, s) in enumerate(calls):
        lead, own = n == 0, n == min(1, len(calls) - 1)
        loading = waiting[: len(waiting) if n == len(calls) - 1 else 1 - lead]
        waiting = waiting[len(loading) :]
        loads = len(loading) + lead
        tabled = lead or own
        operands = in_hbm([tile_table]) * tabled
        operands += in_hbm([grads]) if lead else [order, *in_vmem([grads])]
        operands += in_hbm(loading)
        out_shape = [jax.ShapeDtypeStruct((parts * room * owners,), jnp.int32)] * lead + [packed_shape]
        out_shape += [jax.ShapeDtypeStruct((room * owners,), jnp.int32), slots_shape] * own
        out_shape += [pltpu.VMEM(grads.shape, grads.dtype)] * lead + [f32_tiles] * len(loading)
        result = pl.pallas_call(
            functools.partial(pack_kernel, plan, k, s, lead, own, loads),
            out_shape=out_shape,
            in_specs=[HBM] * tabled + [SMEM, VMEM] * (not lead) + [HBM] * loads,
            out_specs=[SMEM] * lead + [VMEM] + [SMEM, VMEM] * own + [VMEM] * loads,
            scratch_shapes=[pltpu.VMEM((TB * parts, TB), jnp.float32)]
            + [pltpu.SMEM(tile_table.shape, jnp.int32), pltpu.SMEM((owners,), jnp.int32)] * tabled
            + [pltpu.VMEM(tile_table.shape, jnp.int32)] * own
            + [pltpu.SemaphoreType.DMA((max(1, loads * SPLIT + tabled + own),))],
            compiler_params=pltpu.CompilerParams(vmem_limit_bytes=PACK_MIB << 20),
            cost_estimate=pl.CostEstimate(flops=6000000, bytes_accessed=2 << 20, transcendentals=0),
        )(*operands)
        result = list(result)
        if lead:
            order = result.pop(0)
        packed = result.pop(0)
        if own:
            order_own, slots = result.pop(0), result.pop(0)
        if lead:
            grads = result.pop(0)
        states += result
        arrived.setdefault(k, []).append(lax.ppermute(packed, "dp", cycles[s]))

    news = []
    groups = {}
    for k in plan.chunks:
        count = 5 + parts - 1
        apart = parts == 2 and k == 0
        shapes = [block_shape] * plan.near
        if apart:
            shapes[0] = pltpu.VMEM((room * TB, TB), jnp.bfloat16)
            shapes.append(pltpu.VMEM((plan.pad, LANES), jnp.bfloat16))
        results = pl.pallas_call(
            functools.partial(adam_kernel, plan, k, not news),
            out_shape=[f32_tiles] * 3 + shapes,
            in_specs=[SMEM] + [VMEM] * (3 + parts) + [VMEM] * len(news),
            out_specs=[VMEM] * (3 + len(shapes)),
            input_output_aliases={count + j: j for j in range(len(news))},
            scratch_shapes=[pltpu.VMEM((TB * parts, TB), jnp.float32), pltpu.VMEM((entries, 8, LANES), jnp.float32)],
            compiler_params=pltpu.CompilerParams(vmem_limit_bytes=ADAM_MIB << 20),
            cost_estimate=pl.CostEstimate(flops=25000000, bytes_accessed=6 << 20, transcendentals=0),
        )(order_own, *in_vmem([grads, *states]), *arrived[k], *in_vmem(news))
        news, blocks = results[:3], results[3 : 3 + plan.near]
        if apart:
            tail_apart = results[-1]
        groups[k] = []
        for q, block in enumerate(blocks):
            if k or q:
                block = lax.ppermute(block, "shard", plan.pattern(k, q))
            groups[k].append(block)

    entries, stage = [], []
    tails, tail_keys = [], []
    if parts == 2:
        tail_keys = [(k, q) for k in plan.chunks for q in range(plan.near)]
        merges = [keys for keys in MERGES if all(key in tail_keys for key in keys)]
        rest = [key for key in tail_keys if key != (0, 0) and not any(key in keys for keys in merges)]
        merges = [[key] for key in rest] + merges
        for (k, q), block in ((key, groups[key[0]][key[1]]) for key in tail_keys):
            entries.append(((k, q, 0, None), block))
            stage.append(int((k, q) in merges[-1] and len(merges) > 1))
        entries.append(((0, 0, 1, None), lax.ppermute(groups[0][0], "dp", cycles[1])))
        stage.append(0)
        for n, keys in enumerate(merges):
            ends = [tail_apart if key == (0, 0) else groups[key[0]][key[1]] for key in tail_keys]
            ends = ends if n == len(merges) - 1 else []
            merged = pl.pallas_call(
                functools.partial(merge_kernel, plan, len(keys), len(ends)),
                out_shape=[pltpu.VMEM((len(keys) * room * TB, TB), jnp.bfloat16)]
                + [pltpu.VMEM((plan.pad, LANES), jnp.bfloat16)] * bool(ends),
                in_specs=[VMEM] * (len(keys) + len(ends)),
                out_specs=[VMEM] * (1 + bool(ends)),
                compiler_params=pltpu.CompilerParams(vmem_limit_bytes=1 << 20),
                cost_estimate=pl.CostEstimate(flops=1000000, bytes_accessed=1 << 20, transcendentals=0),
            )(*[groups[k][q] for k, q in keys], *ends)
            if ends:
                tails = [merged[1], lax.ppermute(merged[1], "dp", cycles[1])]
            passed = lax.ppermute(merged[0], "dp", cycles[1])
            entries.append(([(k, q, 1, j) for j, (k, q) in enumerate(keys)], passed))
            stage.append(2 if n == len(merges) - 1 else int(n > 0 and len(merges) > 1))
    else:
        keys = [(k, q) for k in plan.chunks for q in range(plan.near)]
        stacked = jnp.stack([block for k in plan.chunks for block in groups[k]])
        for s in range(parts):
            passed = lax.ppermute(stacked, "dp", cycles[s]) if s else stacked
            entries.append(([(k, q, s, n) for n, (k, q) in enumerate(keys)], passed))
        stage = [0] * len(entries)
    saved = []
    for new in news:
        saved.append(
            pl.pallas_call(
                store_kernel,
                out_shape=pltpu.HBM((tiles, TB, TB), jnp.float32),
                in_specs=[VMEM],
                out_specs=HBM,
                scratch_shapes=[pltpu.SemaphoreType.DMA((SPLIT,))],
                compiler_params=pltpu.CompilerParams(vmem_limit_bytes=1 << 20),
                cost_estimate=pl.CostEstimate(flops=2000000, bytes_accessed=2 << 20, transcendentals=0),
            )(*in_vmem([new]))
        )

    tiles_shape = pltpu.HBM((owned, TB, TB), jnp.bfloat16)
    width = (owned + LANES - 1) // LANES * LANES

    def place(at, previous, ends, gathers):
        group = [e for e, level in zip(entries, stage) if level == at]
        first = not previous
        sources = []
        for n, (key, _) in enumerate(group):
            sources += [(n, *each) for each in (key if isinstance(key, list) else [key])]
        operands = [slots, *[a for _, a in group], *ends]
        operands += in_hbm(previous)
        return pl.pallas_call(
            functools.partial(place_kernel, plan, sources, len(group), tail_keys, first, gathers),
            out_shape=[tiles_shape]
            + [jax.ShapeDtypeStruct((1, width), jnp.float32)] * gathers,
            in_specs=[SMEM]
            + [VMEM] * (len(group) + len(ends))
            + [HBM] * len(previous),
            out_specs=[HBM] + [VMEM] * gathers,
            input_output_aliases={} if first else {1 + len(group) + len(ends): 0},
            scratch_shapes=[pltpu.SemaphoreType.DMA((len(sources) * room,))],
            compiler_params=pltpu.CompilerParams(vmem_limit_bytes=24 << 20),
            cost_estimate=pl.CostEstimate(flops=5000000, bytes_accessed=2 << 20, transcendentals=0),
        )(*operands)

    if 1 in stage:
        (tiles_out,) = place(0, [], [], False)
        tiles_out, scales = place(1, [tiles_out], tails, True)
    else:
        tiles_out, scales = place(0, [], tails, True)
    scales_out = scales[0, :owned].astype(jnp.bfloat16)
    if 2 in stage:
        (tiles_out,) = place(2, [tiles_out], [], False)
    return (*[a.reshape(master.shape) for a in saved], tiles_out, scales_out)


def solution(mesh):
    in_specs = (
        P("dp", "shard", None, None),
        P(),
        P("shard", "dp", None),
        P("shard", "dp", None),
        P("shard", "dp", None),
    )
    out_specs = (
        P("shard", "dp", None),
        P("shard", "dp", None),
        P("shard", "dp", None),
        P("shard", None, None),
        P("shard"),
    )

    return jax.shard_map(per_device, mesh=mesh, in_specs=in_specs, out_specs=out_specs, check_vma=False)
```

```python
import functools

import jax
import jax.numpy as jnp
from jax import lax
from jax.experimental import pallas as pl
from jax.experimental.pallas import tpu as pltpu
from jax.sharding import PartitionSpec as P


TB = 128
LANES = 128
UNROLL = 2
SPLIT = 4
MERGES = (
    ((3, 0), (3, 1)),
    ((3, 2), (3, 3)),
    ((1, 0), (1, 1), (1, 2), (1, 3)),
    ((2, 0),),
    ((2, 1), (0, 1)),
    ((2, 2), (2, 3)),
    ((0, 2), (0, 3)),
)
PACK_MIB = 4
ADAM_MIB = 4


beta_first = 0.9
beta_second = 0.95
learning_rate = 0.002
weight_decay = 0.1
adam_epsilon = 1e-08
scale_epsilon = 1e-06
step_count = 10

HBM = pl.BlockSpec(memory_space=pltpu.HBM)
VMEM = pl.BlockSpec(memory_space=pltpu.VMEM)
SMEM = pl.BlockSpec(memory_space=pltpu.SMEM)


def in_hbm(arrays):
    return [pltpu.with_memory_space_constraint(a, pltpu.HBM) for a in arrays]


def in_vmem(arrays):
    return [pltpu.with_memory_space_constraint(a, pltpu.VMEM) for a in arrays]


def extract(raw, wide, part, parts):
    wide[...] = raw[...].astype(jnp.float32)
    return wide[pl.ds(part, TB, stride=parts), :]


def other(index, step, size):
    if size & (size - 1) == 0:
        return index ^ step
    return (index + step) % size


def back(index, step, size):
    if size & (size - 1) == 0:
        return index ^ step
    return (index + size - step) % size


class Plan:
    def __init__(self, parts, owners, owned, tiles):
        self.parts, self.owners, self.owned, self.tiles = parts, owners, owned, tiles
        self.sub_len = owned // parts
        self.room = (self.sub_len + owners - 1) // owners
        self.far = 4 if owners % 4 == 0 and owners > 4 else 1
        self.near = owners // self.far
        self.chunks = [self.far - 1] + list(range(1, self.far - 1)) + [0] if self.far > 1 else [0]
        self.per_chunk = self.near * self.room
        self.pad = (self.room + 7) // 8 * 8
        self.height = self.room * TB + self.pad

    def pattern(self, k, q):
        pairs = []
        for i in range(self.owners):
            far, near = divmod(i, self.near)
            pairs.append((i, other(far, k, self.far) * self.near + other(near, q, self.near)))
        return pairs

    def source(self, me, k, q):
        return back(me // self.near, k, self.far) * self.near + back(me % self.near, q, self.near)


def step_between(here, there, size):
    if size & (size - 1) == 0:
        return here ^ there
    return lax.rem(there + size - here, size)


def fill_order(part, plan, table, order, base, count):
    me = lax.axis_index("shard")
    entries = plan.owners * plan.room

    def clear(j, carry):
        order[base + j] = 0
        return carry

    def zero(j, carry):
        count[j] = 0
        return carry

    def enter(t, carry):
        owner = table[me, part * plan.sub_len + t] // plan.owned
        rank = count[owner]
        count[owner] = rank + 1
        k = step_between(me // plan.near, owner // plan.near, plan.far)
        q = step_between(me % plan.near, owner % plan.near, plan.near)
        order[base + (k * plan.near + q) * plan.room + rank] = t
        return carry

    if entries != plan.sub_len:
        lax.fori_loop(0, entries, clear, 0)
    lax.fori_loop(0, plan.owners, zero, 0, unroll=True)
    lax.fori_loop(0, plan.sub_len, enter, 0, unroll=12)


def find_slots(plan, table, out):
    me = lax.axis_index("shard")
    owned, sub_len = plan.owned, plan.sub_len
    local = table[...] - me * owned
    mine = (local >= 0) & (local < owned)
    before = lax.broadcasted_iota(jnp.int32, (owned, owned), 0)
    after = lax.broadcasted_iota(jnp.int32, (owned, owned), 1)
    same = before // sub_len == after // sub_len
    counts = jnp.where((before < after) & same, 1.0, 0.0).astype(jnp.bfloat16)
    flags = jnp.where(mine, 1.0, 0.0).astype(jnp.bfloat16)
    rank = jnp.dot(flags, counts, preferred_element_type=jnp.float32)
    column = lax.broadcasted_iota(jnp.int32, local.shape, 1) // sub_len
    lane = lax.broadcasted_iota(jnp.int32, out.shape, 1)
    value = jnp.where(mine, local + 1, 0).astype(jnp.float32)
    total = jnp.zeros(out.shape, jnp.float32)
    for part in range(plan.parts):
        for r in range(plan.room):
            chosen = jnp.where((column == part) & (rank == float(r)), value, 0.0)
            found = jnp.sum(chosen, axis=1, keepdims=True)
            total = jnp.where(lane == part * plan.room + r, found, total)
    out[...] = total.astype(jnp.int32) - 1


def pack_kernel(plan, chunk, shift, lead, own, loads, *refs):
    parts, entries, room = plan.parts, plan.per_chunk, plan.room
    here = lax.axis_index("dp")
    part = lax.rem(here + shift, parts)
    refs = list(refs)
    take = lambda n: [refs.pop(0) for _ in range(n)]
    (table,) = take(1) if lead or own else (None,)
    (order,) = take(1) if not lead else (None,)
    (grads,) = take(1) if not lead else (None,)
    sources = take(loads)
    (order,) = take(1) if lead else (order,)
    (out,) = take(1)
    (order_own, slots) = take(2) if own else (None, None)
    targets = take(loads)
    if lead:
        grads = targets[0]
    (wide,) = take(1)
    rows, count = take(2) if lead or own else (None, None)
    (flat,) = take(1) if own else (None,)
    (sems,) = take(1)
    pairs = []
    for a, b in zip(sources, targets):
        size = a.shape[0] // SPLIT
        pairs += [(a.at[pl.ds(n * size, size)], b.at[pl.ds(n * size, size)]) for n in range(SPLIT)]
    loads *= SPLIT
    pairs += [(table, rows)] * bool(lead or own) + [(table, flat)] * bool(own)
    copies = [pltpu.make_async_copy(a, b, sems.at[n]) for n, (a, b) in enumerate(pairs)]
    for copy in copies:
        copy.start()
    entries_of_part = plan.owners * room
    if lead:
        copies[loads].wait()
        fill_order(part, plan, rows, order, part * entries_of_part, count)
        for copy in copies[:loads]:
            copy.wait()
    base = part * entries_of_part + chunk * entries

    def body(i, carry):
        out[i] = extract(grads.at[order[base + i]], wide, part, parts).astype(out.dtype)
        return carry

    lax.fori_loop(0, entries, body, 0, unroll=3)
    if lead:
        for s in range(1, parts - 1):
            later = lax.rem(part + s, parts)
            fill_order(later, plan, rows, order, later * entries_of_part, count)
    if own:
        if not lead:
            copies[loads].wait()
        copies[loads + 1].wait()
        fill_order(here, plan, rows, order_own, 0, count)
        find_slots(plan, flat, slots)
    for n, copy in enumerate(copies):
        if n < loads and not lead:
            copy.wait()


def adam_kernel(plan, chunk, first, *refs):
    parts, entries, room = plan.parts, plan.per_chunk, plan.room
    order, grads, master, moment, second = refs[:5]
    arrived = refs[5 : 4 + parts]
    refs = refs[4 + parts + (0 if first else 3) :]
    master_out, moment_out, second_out = refs[:3]
    blocks = refs[3 : 3 + plan.near]
    apart = refs[3 + plan.near : -2]
    wide, peak = refs[-2:]
    part = lax.axis_index("dp")
    base = chunk * entries
    first_fix = 1.0 / (1.0 - beta_first**step_count)
    second_fix = 1.0 / (1.0 - beta_second**step_count)
    rows = 32

    def update(i, carry):
        tile = order[base + i]
        wide[...] = grads[tile].astype(jnp.float32)
        top = None
        for b in range(0, TB, rows):
            at = pl.ds(b, rows)
            grad = wide[pl.ds(b * parts + part, rows, stride=parts), :]
            for ref in arrived:
                grad = grad + ref[i, at, :].astype(jnp.float32)
            moment_new = beta_first * moment[tile, at, :] + (1.0 - beta_first) * grad
            second_new = beta_second * second[tile, at, :] + (1.0 - beta_second) * grad * grad
            old = master[tile, at, :]
            step = moment_new * first_fix / (jnp.sqrt(second_new * second_fix) + adam_epsilon)
            master_new = old - learning_rate * (step + weight_decay * old)
            master_out[tile, at, :] = master_new
            moment_out[tile, at, :] = moment_new
            second_out[tile, at, :] = second_new
            size = jnp.abs(master_new)
            for s in range(0, rows, 8):
                top = size[s : s + 8] if top is None else jnp.maximum(top, size[s : s + 8])
        peak[i] = top
        return carry

    lax.fori_loop(0, entries, update, 0, unroll=UNROLL)
    largest = jnp.max(jnp.max(peak[...], axis=2, keepdims=True), axis=1, keepdims=True)
    rounded = (largest + scale_epsilon).astype(jnp.bfloat16).astype(jnp.float32)
    peak[...] = jnp.broadcast_to(rounded, peak.shape)
    row = lax.broadcasted_iota(jnp.int32, (plan.pad, LANES), 0)
    for q, block in enumerate(blocks):
        tail = jnp.zeros((plan.pad, LANES), jnp.float32)
        for r in range(room):
            i = q * room + r
            tile = order[base + i]
            scale = peak[i]
            inverse = 1.0 / scale
            tail = jnp.where(row == r, jnp.concatenate([scale] * (plan.pad // 8), axis=0), tail)
            for b in range(0, TB, 16):
                pair = [master_out[tile, pl.ds(b + s, 8), :] * inverse for s in (0, 8)]
                block[pl.ds(r * TB + b, 16), :] = jnp.concatenate(pair, axis=0).astype(block.dtype)
        if q == 0 and apart:
            apart[0][...] = tail.astype(block.dtype)
        else:
            block[pl.ds(room * TB, plan.pad), :] = tail.astype(block.dtype)


def store_kernel(held, saved, sems):
    size = held.shape[0] // SPLIT
    copies = []
    for n in range(SPLIT):
        piece = pl.ds(n * size, size)
        copies.append(pltpu.make_async_copy(held.at[piece], saved.at[piece], sems.at[n]))
    for copy in copies:
        copy.start()
    for copy in copies:
        copy.wait()


def merge_kernel(plan, count, ends, *refs):
    blocks, tails = refs[:count], refs[count : count + ends]
    rows = plan.room * TB
    for n, block in enumerate(blocks):
        refs[count + ends][pl.ds(n * rows, rows), :] = block[pl.ds(0, rows), :]
    if ends:
        out = refs[-1]
        group = lax.broadcasted_iota(jnp.int32, out.shape, 1) // (LANES // ends)
        total = jnp.zeros(out.shape, jnp.float32)
        for n, ref in enumerate(tails):
            tail = ref[pl.ds(ref.shape[0] - plan.pad, plan.pad), :].astype(jnp.float32)
            total = jnp.where(group == n, tail, total)
        out[...] = total.astype(out.dtype)


def place_kernel(plan, sources, count, keys, first, gathers, *refs):
    room = plan.room
    refs = list(refs)
    take = lambda n: [refs.pop(0) for _ in range(n)]
    (slots,), blocks = take(1), take(count)
    late = take(plan.parts) if gathers and keys else []
    if not first:
        take(1)
    (tiles_out,) = take(1)
    (scales_out,) = take(1) if gathers else (None,)
    (sems,) = take(1)
    here, me = lax.axis_index("dp"), lax.axis_index("shard")

    def slot_of(k, q, shift, r):
        part = lax.rem(here + plan.parts - shift, plan.parts)
        return slots[plan.source(me, k, q), part * room + r]

    entries, views = [], []
    for n, (ref, k, q, shift, at) in enumerate(sources):
        stacked = len(blocks[ref].shape) == 3
        views.append(blocks[ref].at[at] if stacked else blocks[ref])
        start = 0 if stacked or at is None else at * room * TB
        for r in range(room):
            slot = slot_of(k, q, shift, r)
            copy = pltpu.make_async_copy(views[n].at[pl.ds(start + r * TB, TB)], tiles_out.at[slot], sems.at[n * room + r])
            entries.append((slot, copy))
            if room * plan.owners == plan.sub_len:
                copy.start()
            else:
                pl.when(slot >= 0)(copy.start)
    if gathers:
        lane = lax.broadcasted_iota(jnp.int32, scales_out.shape, 1)
        total = jnp.zeros(scales_out.shape, jnp.float32)
        ends = []
        if keys:
            for shift, ref in enumerate(late):
                packed = ref[...].astype(jnp.float32)
                for n, (k, q) in enumerate(keys):
                    at = n * (LANES // len(keys))
                    ends.append((jnp.broadcast_to(packed[:, at : at + 1], packed.shape), (k, q, shift)))
        else:
            ends = [(view[pl.ds(room * TB, plan.pad), :], key[1:4]) for view, key in zip(views, sources)]
        for rows, (k, q, shift) in ends:
            for r in range(room):
                wide = jnp.concatenate([rows[r : r + 1].astype(jnp.float32)] * (scales_out.shape[1] // LANES), axis=1)
                total = jnp.where(lane == slot_of(k, q, shift, r), wide, total)
        scales_out[...] = total
    for slot, copy in entries:
        if room * plan.owners == plan.sub_len:
            copy.wait()
        else:
            pl.when(slot >= 0)(copy.wait)


def per_device(gradients, tile_table, master, moment, second):
    owners = lax.axis_size("shard")
    parts = lax.axis_size("dp")
    owned = tile_table.shape[1]
    tiles = master.size // (TB * TB)
    plan = Plan(parts, owners, owned, tiles)
    room, entries = plan.room, plan.per_chunk

    grads = gradients.reshape(parts, tiles, TB, TB).transpose(1, 2, 0, 3).reshape(tiles, TB * parts, TB)
    states = [a.reshape(tiles, TB, TB) for a in (master, moment, second)]
    cycles = {s: [(d, (d + s) % parts) for d in range(parts)] for s in range(1, parts)}
    f32_tiles = pltpu.VMEM((tiles, TB, TB), jnp.float32)
    block_shape = pltpu.VMEM((plan.height, TB), jnp.bfloat16)

    order = None
    waiting = list(states)
    states = []
    arrived = {}
    calls = [(k, s) for k in plan.chunks for s in range(1, parts)]
    packed_shape = pltpu.VMEM((entries, TB, TB), jnp.bfloat16)
    slots_shape = jax.ShapeDtypeStruct((owners, (parts * room + LANES - 1) // LANES * LANES), jnp.int32)
    for n, (k, s) in enumerate(calls):
        lead, own = n == 0, n == min(1, len(calls) - 1)
        loading = waiting[: len(waiting) if n == len(calls) - 1 else 1 - lead]
        waiting = waiting[len(loading) :]
        loads = len(loading) + lead
        tabled = lead or own
        operands = in_hbm([tile_table]) * tabled
        operands += in_hbm([grads]) if lead else [order, *in_vmem([grads])]
        operands += in_hbm(loading)
        out_shape = [jax.ShapeDtypeStruct((parts * room * owners,), jnp.int32)] * lead + [packed_shape]
        out_shape += [jax.ShapeDtypeStruct((room * owners,), jnp.int32), slots_shape] * own
        out_shape += [pltpu.VMEM(grads.shape, grads.dtype)] * lead + [f32_tiles] * len(loading)
        result = pl.pallas_call(
            functools.partial(pack_kernel, plan, k, s, lead, own, loads),
            out_shape=out_shape,
            in_specs=[HBM] * tabled + [SMEM, VMEM] * (not lead) + [HBM] * loads,
            out_specs=[SMEM] * lead + [VMEM] + [SMEM, VMEM] * own + [VMEM] * loads,
            scratch_shapes=[pltpu.VMEM((TB * parts, TB), jnp.float32)]
            + [pltpu.SMEM(tile_table.shape, jnp.int32), pltpu.SMEM((owners,), jnp.int32)] * tabled
            + [pltpu.VMEM(tile_table.shape, jnp.int32)] * own
            + [pltpu.SemaphoreType.DMA((max(1, loads * SPLIT + tabled + own),))],
            compiler_params=pltpu.CompilerParams(vmem_limit_bytes=PACK_MIB << 20),
            cost_estimate=pl.CostEstimate(flops=6000000, bytes_accessed=2 << 20, transcendentals=0),
        )(*operands)
        result = list(result)
        if lead:
            order = result.pop(0)
        packed = result.pop(0)
        if own:
            order_own, slots = result.pop(0), result.pop(0)
        if lead:
            grads = result.pop(0)
        states += result
        arrived.setdefault(k, []).append(lax.ppermute(packed, "dp", cycles[s]))

    news = []
    groups = {}
    for k in plan.chunks:
        count = 5 + parts - 1
        apart = parts == 2 and k == 0
        shapes = [block_shape] * plan.near
        if apart:
            shapes[0] = pltpu.VMEM((room * TB, TB), jnp.bfloat16)
            shapes.append(pltpu.VMEM((plan.pad, LANES), jnp.bfloat16))
        results = pl.pallas_call(
            functools.partial(adam_kernel, plan, k, not news),
            out_shape=[f32_tiles] * 3 + shapes,
            in_specs=[SMEM] + [VMEM] * (3 + parts) + [VMEM] * len(news),
            out_specs=[VMEM] * (3 + len(shapes)),
            input_output_aliases={count + j: j for j in range(len(news))},
            scratch_shapes=[pltpu.VMEM((TB * parts, TB), jnp.float32), pltpu.VMEM((entries, 8, LANES), jnp.float32)],
            compiler_params=pltpu.CompilerParams(vmem_limit_bytes=ADAM_MIB << 20),
            cost_estimate=pl.CostEstimate(flops=25000000, bytes_accessed=6 << 20, transcendentals=0),
        )(order_own, *in_vmem([grads, *states]), *arrived[k], *in_vmem(news))
        news, blocks = results[:3], results[3 : 3 + plan.near]
        if apart:
            tail_apart = results[-1]
        groups[k] = []
        for q, block in enumerate(blocks):
            if k or q:
                block = lax.ppermute(block, "shard", plan.pattern(k, q))
            groups[k].append(block)

    entries, stage = [], []
    tails, tail_keys = [], []
    if parts == 2:
        tail_keys = [(k, q) for k in plan.chunks for q in range(plan.near)]
        merges = [keys for keys in MERGES if all(key in tail_keys for key in keys)]
        rest = [key for key in tail_keys if key != (0, 0) and not any(key in keys for keys in merges)]
        merges = [[key] for key in rest] + merges
        for (k, q), block in ((key, groups[key[0]][key[1]]) for key in tail_keys):
            entries.append(((k, q, 0, None), block))
            stage.append(int((k, q) in merges[-1] and len(merges) > 1))
        entries.append(((0, 0, 1, None), lax.ppermute(groups[0][0], "dp", cycles[1])))
        stage.append(0)
        for n, keys in enumerate(merges):
            ends = [tail_apart if key == (0, 0) else groups[key[0]][key[1]] for key in tail_keys]
            ends = ends if n == len(merges) - 1 else []
            merged = pl.pallas_call(
                functools.partial(merge_kernel, plan, len(keys), len(ends)),
                out_shape=[pltpu.VMEM((len(keys) * room * TB, TB), jnp.bfloat16)]
                + [pltpu.VMEM((plan.pad, LANES), jnp.bfloat16)] * bool(ends),
                in_specs=[VMEM] * (len(keys) + len(ends)),
                out_specs=[VMEM] * (1 + bool(ends)),
                compiler_params=pltpu.CompilerParams(vmem_limit_bytes=1 << 20),
                cost_estimate=pl.CostEstimate(flops=1000000, bytes_accessed=1 << 20, transcendentals=0),
            )(*[groups[k][q] for k, q in keys], *ends)
            if ends:
                tails = [merged[1], lax.ppermute(merged[1], "dp", cycles[1])]
            passed = lax.ppermute(merged[0], "dp", cycles[1])
            entries.append(([(k, q, 1, j) for j, (k, q) in enumerate(keys)], passed))
            stage.append(2 if n == len(merges) - 1 else int(n > len(merges) - 5 and len(merges) > 1))
    else:
        keys = [(k, q) for k in plan.chunks for q in range(plan.near)]
        stacked = jnp.stack([block for k in plan.chunks for block in groups[k]])
        for s in range(parts):
            passed = lax.ppermute(stacked, "dp", cycles[s]) if s else stacked
            entries.append(([(k, q, s, n) for n, (k, q) in enumerate(keys)], passed))
        stage = [0] * len(entries)
    saved = []
    for new in news:
        saved.append(
            pl.pallas_call(
                store_kernel,
                out_shape=pltpu.HBM((tiles, TB, TB), jnp.float32),
                in_specs=[VMEM],
                out_specs=HBM,
                scratch_shapes=[pltpu.SemaphoreType.DMA((SPLIT,))],
                compiler_params=pltpu.CompilerParams(vmem_limit_bytes=1 << 20),
                cost_estimate=pl.CostEstimate(flops=2000000, bytes_accessed=2 << 20, transcendentals=0),
            )(*in_vmem([new]))
        )

    tiles_shape = pltpu.HBM((owned, TB, TB), jnp.bfloat16)
    width = (owned + LANES - 1) // LANES * LANES

    def place(at, previous, ends, gathers):
        group = [e for e, level in zip(entries, stage) if level == at]
        first = not previous
        sources = []
        for n, (key, _) in enumerate(group):
            sources += [(n, *each) for each in (key if isinstance(key, list) else [key])]
        operands = [slots, *[a for _, a in group], *ends]
        operands += in_hbm(previous)
        return pl.pallas_call(
            functools.partial(place_kernel, plan, sources, len(group), tail_keys, first, gathers),
            out_shape=[tiles_shape]
            + [jax.ShapeDtypeStruct((1, width), jnp.float32)] * gathers,
            in_specs=[SMEM]
            + [VMEM] * (len(group) + len(ends))
            + [HBM] * len(previous),
            out_specs=[HBM] + [VMEM] * gathers,
            input_output_aliases={} if first else {1 + len(group) + len(ends): 0},
            scratch_shapes=[pltpu.SemaphoreType.DMA((len(sources) * room,))],
            compiler_params=pltpu.CompilerParams(vmem_limit_bytes=24 << 20),
            cost_estimate=pl.CostEstimate(flops=5000000, bytes_accessed=2 << 20, transcendentals=0),
        )(*operands)

    if 1 in stage:
        (tiles_out,) = place(0, [], [], False)
        tiles_out, scales = place(1, [tiles_out], tails, True)
    else:
        tiles_out, scales = place(0, [], tails, True)
    scales_out = scales[0, :owned].astype(jnp.bfloat16)
    if 2 in stage:
        (tiles_out,) = place(2, [tiles_out], [], False)
    return (*[a.reshape(master.shape) for a in saved], tiles_out, scales_out)


def solution(mesh):
    in_specs = (
        P("dp", "shard", None, None),
        P(),
        P("shard", "dp", None),
        P("shard", "dp", None),
        P("shard", "dp", None),
    )
    out_specs = (
        P("shard", "dp", None),
        P("shard", "dp", None),
        P("shard", "dp", None),
        P("shard", None, None),
        P("shard"),
    )

    return jax.shard_map(per_device, mesh=mesh, in_specs=in_specs, out_specs=out_specs, check_vma=False)
```
